256 devices in a mesh: vert: 16 (over x, y), feat: 16 (over z, core).
Axes of the slice: x: 4, y: 4, z: 8, core: 2. Of those that a mesh axis runs over, the one named last changes fastest.
Arguments:
- features: bfloat16 [131072, 256], P('vert', 'feat'), may hold values from -6 to 6
- tiles: bfloat16 [1024, 16, 128, 128], P('vert'), may hold values from -0.1875 to 0.1875
- tile_cols: int32 [1024, 16], P('vert'), may hold values from 0 to 127
- tile_count: int32 [1024], P('vert'), may hold values from 1 to 16, as said below
- send_list: int32 [16, 16, 4], P('vert'), may hold values from 0 to 63
- weight: bfloat16 [256, 256], replicated, may hold values from -0.375 to 0.375
- bias: float32 [256], replicated, may hold values from -3 to 3
Outputs:
- node_out: bfloat16 [131072, 256], P(('vert', 'feat'))
The draws below stay inside these ranges and needn't reach their ends.
Inputs may be any that keep to these rules, and one draw needn't show every extreme that they name: Row block r uses tile places 0 to tile_count[r] - 1; in every draw some row block uses all 16.
All inputs are finite; a program needn't handle non-finite values.
Results may differ from the reference program's by a relative error of at most 0.0044.
Values may be sent and summed in bfloat16 or wider, within the bound.
No kernel may reach another device: no remote copies, remote signals or barrier semaphores. Data moves between devices by JAX's collectives and lax.ppermute only.
A program may use at most 128 MiB of HBM per device.

```python
import jax
import jax.numpy as jnp
from jax import lax

F = 256
BLK = 128
K = 16
SLOTS = 4
RB_DEV = 64
NRB = 1024
NV = 131072
N_VERT = 16


def draw_tile_count(key, part):
    total = RB_DEV * N_VERT
    row_index = jnp.arange(total, dtype=jnp.int32)
    rank = row_index // RB_DEV
    ceiling = 1 + (K - 1) * (rank + 1) // N_VERT
    picks = jax.random.randint(key, (total,), 0, 1 << 20)
    counts = 1 + picks % ceiling
    chosen = jax.random.randint(jax.random.fold_in(key, 7), (), 0, total)
    return jnp.where(row_index == chosen, K, counts).astype(jnp.int32)


def with_ends(values, rng, least, top_value):
    spot = [jax.random.randint(jax.random.fold_in(rng, axis), (), 0, length) for axis, length in enumerate(values.shape)]
    longest = values.shape.index(max(values.shape))
    next_to = spot[:longest] + [(spot[longest] + 1) % values.shape[longest]] + spot[longest + 1:]
    return values.at[tuple(spot)].set(least).at[tuple(next_to)].set(top_value)


def block_levels(stream_key, dims, split, smallest, top_value):
    gain, own = 1.0, jax.random.fold_in(stream_key, 6)
    for dim, parts in split:
        steps = jnp.exp(jax.random.uniform(jax.random.fold_in(own, dim), (parts,), jnp.float32, smallest / len(split), top_value / len(split)))
        gain = gain * jnp.repeat(steps, dims[dim] // parts).reshape([-1 if axis == dim else 1 for axis in range(len(dims))])
    return gain


def scatter_about(rng, shape, width, reach, cuts=(), held_as=jnp.bfloat16):
    array = jax.random.normal(rng, shape, jnp.float32) * width
    if len(cuts) > 0:
        array = block_levels(rng, shape, cuts, -0.22, 0.18) * array
    return jnp.clip(array, min=-reach, max=reach).astype(held_as)


def setup_inputs(seed: int = 0) -> dict:
    streams_of = jax.random.split(jax.random.key(seed), 8)
    features = scatter_about(streams_of[0], (NV, F), 1.0, 6.0, ((0, 16), (1, 16)))
    tiles = scatter_about(streams_of[1], (NRB, K, BLK, BLK), (BLK * K // 2) ** -0.5, 0.1875, ((0, 16),))
    tile_cols = with_ends(jax.random.randint(streams_of[2], (NRB, K), 0, RB_DEV + N_VERT * SLOTS), jax.random.fold_in(streams_of[2], 1), 0, (RB_DEV + N_VERT * SLOTS) - 1).astype(jnp.int32)
    tile_count = draw_tile_count(jax.random.fold_in(streams_of[7], 71), 0)
    send_list = with_ends(jax.random.randint(streams_of[4], (N_VERT, N_VERT, SLOTS), 0, RB_DEV), jax.random.fold_in(streams_of[4], 1), 0, RB_DEV - 1).astype(jnp.int32)
    weight = scatter_about(streams_of[5], (F, F), F ** -0.5, 0.375)
    bias = scatter_about(streams_of[6], (F,), 0.5, 3.0, (), jnp.float32)
    return dict(features=features, tiles=tiles, tile_cols=tile_cols, tile_count=tile_count, send_list=send_list, weight=weight, bias=bias)


def reference(features, tiles, tile_cols, tile_count, send_list, weight, bias):
    row_owner = jnp.arange(RB_DEV * N_VERT, dtype=jnp.int32) // RB_DEV
    is_local = tile_cols < RB_DEV
    halo_slot = jnp.maximum(tile_cols - RB_DEV, 0)
    source = (halo_slot // SLOTS).astype(jnp.int32)
    position = (halo_slot % SLOTS).astype(jnp.int32)
    sent_block = send_list[source, row_owner[:, None], position]
    column = jnp.where(is_local, row_owner[:, None] * RB_DEV + tile_cols, source * RB_DEV + sent_block).astype(jnp.int32)
    blocks = features.reshape(RB_DEV * N_VERT, BLK, F)
    is_live = jnp.arange(K, dtype=jnp.int32)[None, :] < tile_count[:, None]

    def one_block(block_item):
        tile_row, col_row, live_row = block_item
        picked = blocks[col_row].astype(jnp.float32)
        products = jnp.einsum("kij,kjc->kic", tile_row.astype(jnp.float32), picked)
        kept = jnp.where(live_row[:, None, None], products, jnp.float32(0.0))
        return jnp.sum(kept, axis=0).astype(jnp.bfloat16)

    aggregated = lax.map(one_block, (tiles, column, is_live)).reshape(RB_DEV * N_VERT * BLK, F)
    mixed_rows = jnp.dot(aggregated, weight, preferred_element_type=jnp.float32) + bias
    return jnp.maximum(mixed_rows, jnp.float32(0.0)).astype(jnp.bfloat16)
```

```python
import functools

import jax
import jax.numpy as jnp
from jax import lax
from jax.experimental import pallas as pl
from jax.experimental.pallas import tpu as pltpu
from jax.sharding import PartitionSpec as P

VMEM = pltpu.VMEM
SMEM = pltpu.SMEM
UNROLL = 16
AHEAD = 4
PAIRS_MAX = 8
ROWS = 64
ZERO_SLOT = 64
PAD_ITEM = ((ROWS - 1) << 4) | (ZERO_SLOT << 10) | (ZERO_SLOT << 17)
CHUNKS_MAX = ROWS * PAIRS_MAX // UNROLL
LIST_LEN = ROWS * PAIRS_MAX + PAIRS_MAX + UNROLL + 8


def pick_kernel(send_ref, feat_ref, out_ref):
    slots, peers = send_ref.shape
    for peer in range(peers):
        for slot in range(slots):
            start = pl.multiple_of(send_ref[slot, peer] * 128, 128)
            out_ref[peer * slots + slot] = feat_ref[:, pl.ds(start, 128)]


def run_pairs(list_ref, count, tiles_ref, buf_ref, sem, slab_ref, acc_ref):
    chunks = (count + (UNROLL - 1)) // UNROLL

    def issue(i, carry):
        base = i * UNROLL
        for u in range(UNROLL):
            item = list_ref[base + u]
            ta = item & 1023
            tb = (item & 1008) | (item >> 24)
            at = 2 * (base + u)
            pltpu.make_async_copy(tiles_ref.at[ta], buf_ref.at[at], sem.at[i]).start()
            pltpu.make_async_copy(tiles_ref.at[tb], buf_ref.at[at + 1], sem.at[i]).start()
        return carry

    lax.fori_loop(0, jnp.minimum(chunks, AHEAD), issue, 0)

    def chunk(i, carry):
        base = i * UNROLL
        landed = buf_ref.at[pl.ds(2 * base, 2 * UNROLL)]
        pltpu.make_async_copy(tiles_ref.at[pl.ds(0, 2 * UNROLL)], landed, sem.at[i]).wait()

        @pl.when(i + AHEAD < chunks)
        def _():
            issue(i + AHEAD, 0)

        for u in range(UNROLL):
            item = list_ref[base + u]
            row = (item >> 4) & 63
            xa = (item >> 10) & 127
            xb = (item >> 17) & 127
            at = 2 * (base + u)
            tile = jnp.concatenate([buf_ref[at], buf_ref[at + 1]], axis=1)
            slab = jnp.concatenate([slab_ref[xa], slab_ref[xb]], axis=1)
            acc_ref[row] += lax.dot_general(
                slab, tile, (((1,), (1,)), ((), ())), preferred_element_type=jnp.float32
            )
        return carry

    lax.fori_loop(0, chunks, chunk, 0)


def local_kernel(
    tiles_ref, cols_ref, count_ref, feat_ref,
    acc_ref, halo_ref,
    buf_ref, slab_ref, table_vmem, table_ref, local_ref, load_sem, table_sem,
):
    counts = count_ref[...]
    places = cols_ref.shape[0]
    rank = lax.broadcasted_iota(jnp.int32, (places, ROWS), 0)
    empty = jnp.full((places, ROWS), ZERO_SLOT, jnp.int32)
    codes = [empty, empty]
    seen = [jnp.zeros((1, ROWS), jnp.int32), jnp.zeros((1, ROWS), jnp.int32)]
    for k in range(places):
        col = cols_ref[k:k + 1, :]
        for part in range(2):
            kept = (col < ROWS) if part == 0 else (col >= ROWS)
            kept = kept & (counts > k)
            code = (col - part * ROWS) + (k << 7)
            codes[part] = jnp.where((rank == seen[part]) & kept, code, codes[part])
            seen[part] = seen[part] + kept.astype(jnp.int32)
    rows = lax.broadcasted_iota(jnp.int32, (1, ROWS), 1)
    for part in range(2):
        for p in range(PAIRS_MAX):
            a = codes[part][2 * p:2 * p + 1, :]
            b = codes[part][2 * p + 1:2 * p + 2, :]
            item = (a >> 7) | (rows << 4) | ((a & 127) << 10) | ((b & 127) << 17) | ((b >> 7) << 24)
            at = part * PAIRS_MAX + p
            table_vmem[at:at + 1, 0:ROWS] = item
        at = 2 * PAIRS_MAX + part
        table_vmem[at:at + 1, 0:ROWS] = (seen[part] + 1) >> 1
    to_smem = pltpu.make_async_copy(table_vmem, table_ref, table_sem)
    to_smem.start()

    acc_ref[...] = jnp.zeros(acc_ref.shape, jnp.float32)
    for r in range(ROWS):
        slab_ref[r] = feat_ref[:, r * 128:(r + 1) * 128]
    slab_ref[ZERO_SLOT] = jnp.zeros(slab_ref.shape[1:], slab_ref.dtype)
    to_smem.wait()

    def flatten(part, out_ref):
        def one_row(r, n):
            for p in range(PAIRS_MAX):
                out_ref[n + p] = table_ref[part * PAIRS_MAX + p, r]
            return n + table_ref[2 * PAIRS_MAX + part, r]

        n = lax.fori_loop(0, ROWS, one_row, jnp.int32(0), unroll=2)
        for u in range(UNROLL):
            out_ref[n + u] = PAD_ITEM
        return n

    n_local = flatten(0, local_ref)
    run_pairs(local_ref, n_local, tiles_ref, buf_ref, load_sem, slab_ref, acc_ref)
    halo_ref[LIST_LEN - 1] = flatten(1, halo_ref)


def halo_kernel(
    halo_ref, tiles_ref, part_ref, arrived_ref, out_ref, buf_ref, slab_ref, acc_ref, load_sem
):
    acc_ref[...] = part_ref[...]
    for s in range(arrived_ref.shape[0]):
        slab_ref[s] = arrived_ref[s]
    slab_ref[ZERO_SLOT] = jnp.zeros(slab_ref.shape[1:], slab_ref.dtype)
    n_halo = halo_ref[LIST_LEN - 1]
    run_pairs(halo_ref, n_halo, tiles_ref, buf_ref, load_sem, slab_ref, acc_ref)
    owners = out_ref.shape[0]
    each = ROWS // owners
    for owner in range(owners):
        for j in range(each):
            out_ref[owner, :, j * 128:(j + 1) * 128] = acc_ref[owner * each + j].astype(out_ref.dtype)


def per_device(features, tiles, tile_cols, tile_count, send_list, weight, bias):
    block_count, tile_depth, edge, _ = tiles.shape
    width = features.shape[1]
    feat_count = lax.axis_size("feat")
    bf16, f32 = jnp.bfloat16, jnp.float32
    feat_t = features.T
    whole = pl.BlockSpec(memory_space=VMEM)
    scalar = pl.BlockSpec(memory_space=SMEM)

    chosen = pl.pallas_call(
        pick_kernel,
        out_shape=jax.ShapeDtypeStruct((block_count, width, edge), bf16),
        in_specs=[scalar, whole],
        out_specs=whole,
        name="pick",
        cost_estimate=pl.CostEstimate(flops=1000, bytes_accessed=500000, transcendentals=0),
    )(send_list[0].T, feat_t)
    arrived = lax.all_to_all(
        chosen.reshape(16, 4, width, edge), "vert", split_axis=0, concat_axis=0, tiled=True
    ).reshape(block_count, width, edge)

    flat_tiles = tiles.reshape(block_count * tile_depth, edge, edge)
    in_hbm = pl.BlockSpec(memory_space=pl.ANY)
    buffers = [
        VMEM((2 * UNROLL * CHUNKS_MAX, edge, edge), bf16),
        VMEM((ZERO_SLOT + 1, width, edge), bf16),
    ]
    part, halo = pl.pallas_call(
        local_kernel,
        out_shape=(
            jax.ShapeDtypeStruct((block_count, width, edge), f32),
            jax.ShapeDtypeStruct((LIST_LEN,), jnp.int32),
        ),
        in_specs=[in_hbm, whole, whole, whole],
        out_specs=(whole, scalar),
        scratch_shapes=buffers + [
            VMEM((24, 128), jnp.int32),
            SMEM((24, 128), jnp.int32),
            SMEM((LIST_LEN,), jnp.int32),
            pltpu.SemaphoreType.DMA((CHUNKS_MAX,)),
            pltpu.SemaphoreType.DMA,
        ],
        name="local",
        compiler_params=pltpu.CompilerParams(vmem_limit_bytes=44 * 1024 * 1024),
        cost_estimate=pl.CostEstimate(
            flops=8_000_000_000, bytes_accessed=17_000_000, transcendentals=0
        ),
    )(flat_tiles, tile_cols.T, tile_count.reshape(1, block_count), feat_t)

    hidden = pl.pallas_call(
        halo_kernel,
        out_shape=jax.ShapeDtypeStruct((feat_count, width, block_count * edge // feat_count), bf16),
        in_specs=[scalar, in_hbm, whole, whole],
        out_specs=whole,
        scratch_shapes=buffers + [
            VMEM((block_count, width, edge), f32),
            pltpu.SemaphoreType.DMA((CHUNKS_MAX,)),
        ],
        name="halo",
        compiler_params=pltpu.CompilerParams(vmem_limit_bytes=44 * 1024 * 1024),
        cost_estimate=pl.CostEstimate(
            flops=3_000_000_000, bytes_accessed=17_000_000, transcendentals=0
        ),
    )(halo, flat_tiles, part, arrived)

    full_rows = lax.all_to_all(hidden, "feat", split_axis=0, concat_axis=0, tiled=True)
    full_rows = full_rows.reshape(feat_count * width, -1)
    mixed_rows = lax.dot_general(
        full_rows, weight, (((0,), (0,)), ((), ())), preferred_element_type=f32
    )
    return jnp.maximum(mixed_rows + bias, f32(0.0)).astype(bf16)


def solution(mesh):
    return jax.shard_map(
        per_device,
        mesh=mesh,
        in_specs=(
            P("vert", "feat"),
            P("vert", None, None, None),
            P("vert", None),
            P("vert"),
            P("vert", None, None),
            P(),
            P(),
        ),
        out_specs=P(("vert", "feat"), None),
        check_vma=False,
    )
```

```python
import jax
import jax.numpy as jnp
from jax import lax
from jax.experimental import pallas as pl
from jax.experimental.pallas import tpu as pltpu
from jax.sharding import PartitionSpec as P

VMEM = pltpu.VMEM
SMEM = pltpu.SMEM
UNROLL = 32
AHEAD = 2
PAIRS_MAX = 8
ROWS = 64
EDGE = 128
SLOTS = ROWS + 1
CHUNKS_MAX = ROWS * PAIRS_MAX // UNROLL
LIST_ROWS = 8
LIST_SPAN = 5 * 128
TOTAL_ROW = 5


def pick_kernel(send_ref, feat_hbm, cols_hbm, count_hbm, out_ref, slab_ref, cols_ref, count_ref, feat_ref, sem):
    copies = [
        pltpu.make_async_copy(src, dst, sem.at[i])
        for i, (src, dst) in enumerate(
            [(feat_hbm, feat_ref), (cols_hbm, cols_ref), (count_hbm, count_ref)]
        )
    ]
    for copy in copies:
        copy.start()
    copies[0].wait()
    slots, peers = send_ref.shape
    for peer in range(peers):
        for slot in range(slots):
            start = pl.multiple_of(send_ref[slot, peer] * EDGE, EDGE)
            out_ref[peer * slots + slot] = feat_ref[:, pl.ds(start, EDGE)]
    slab_ref[0] = jnp.zeros(slab_ref.shape[1:], slab_ref.dtype)
    for r in range(ROWS):
        slab_ref[r + 1] = feat_ref[:, r * EDGE:(r + 1) * EDGE]
    copies[1].wait()
    copies[2].wait()


def item_at(list_ref, i):
    return list_ref[i >> 7, i & 127]


def issue(list_ref, i, tiles_ref, buf_ref, at, sem):
    for u in range(UNROLL):
        item = item_at(list_ref, i * UNROLL + u)
        ta = item & 1023
        tb = (item & 1008) | (item >> 24)
        pltpu.make_async_copy(tiles_ref.at[ta], buf_ref.at[at + 2 * u], sem).start()
        pltpu.make_async_copy(tiles_ref.at[tb], buf_ref.at[at + 2 * u + 1], sem).start()


def landed(tiles_ref, buf_ref, at, sem):
    pltpu.make_async_copy(
        tiles_ref.at[pl.ds(0, 2 * UNROLL)], buf_ref.at[pl.ds(at, 2 * UNROLL)], sem
    ).wait()


def add_chunk(list_ref, i, buf_ref, at, slab_ref, acc_ref):
    for u in range(UNROLL):
        item = item_at(list_ref, i * UNROLL + u)
        row = (item >> 4) & 63
        xa = (item >> 10) & 127
        xb = (item >> 17) & 127
        tile = jnp.concatenate([buf_ref[at + 2 * u], buf_ref[at + 2 * u + 1]], axis=1)
        slab = jnp.concatenate([slab_ref[xa], slab_ref[xb]], axis=1)
        acc_ref[row] += lax.dot_general(
            slab, tile, (((1,), (1,)), ((), ())), preferred_element_type=jnp.float32
        )


def run_chunks(list_ref, first, chunks, tiles_ref, buf_ref, sem, slab_ref, acc_ref):
    def one(i, carry):
        at = i * (2 * UNROLL)
        landed(tiles_ref, buf_ref, at, sem.at[i])

        @pl.when(i + AHEAD < chunks)
        def _():
            issue(list_ref, i + AHEAD, tiles_ref, buf_ref, at + AHEAD * 2 * UNROLL, sem.at[i + AHEAD])

        add_chunk(list_ref, i, buf_ref, at, slab_ref, acc_ref)
        return carry

    lax.fori_loop(first, chunks, one, 0)


def issue_first(list_ref, first, chunks, tiles_ref, buf_ref, sem):
    def one(i, carry):
        issue(list_ref, i, tiles_ref, buf_ref, i * (2 * UNROLL), sem.at[i])
        return carry

    lax.fori_loop(first, jnp.minimum(chunks, first + AHEAD), one, 0)


def chunk_count(list_ref):
    return (list_ref[TOTAL_ROW, 127] + (UNROLL - 1)) // UNROLL


def build_lists(cols_ref, count_ref, piece_ref, halo_table_ref, local_table_ref):
    f32, i32, bf16 = jnp.float32, jnp.int32, jnp.bfloat16
    counts = count_ref[...]
    places = cols_ref.shape[0]
    rank = lax.broadcasted_iota(i32, (places, ROWS), 0)
    codes = [jnp.zeros((places, ROWS), i32)] * 2
    seen = [jnp.zeros((1, ROWS), i32)] * 2
    for k in range(places):
        col = cols_ref[k:k + 1, :]
        for part in range(2):
            kept = (col < ROWS) if part == 0 else (col >= ROWS)
            kept = kept & (counts > k)
            code = (col - part * ROWS + 1) + (k << 7)
            codes[part] = jnp.where((rank == seen[part]) & kept, code, codes[part])
            seen[part] = seen[part] + kept.astype(i32)
    lane_row = lax.broadcasted_iota(i32, (1, ROWS), 1)
    for part in range(2):
        base = part * 32
        for p in range(PAIRS_MAX):
            a = codes[part][2 * p:2 * p + 1, :]
            b = codes[part][2 * p + 1:2 * p + 2, :]
            piece_ref[base + p:base + p + 1, :] = ((a >> 7) | ((b >> 7) << 4)).astype(f32)
            piece_ref[base + 8 + p:base + 9 + p, :] = (a & 127).astype(f32)
            piece_ref[base + 16 + p:base + 17 + p, :] = (b & 127).astype(f32)
        piece_ref[base + 24:base + 25, :] = lane_row.astype(f32)
        piece_ref[base + 25:base + 32, :] = jnp.zeros((7, ROWS), f32)
        piece_ref[64 + part:65 + part, :] = ((seen[part] + 1) >> 1).astype(f32)
    piece_ref[66:72, :] = jnp.zeros((6, ROWS), f32)

    pairs = piece_ref[64:72, :].astype(bf16)
    r_out = lax.broadcasted_iota(i32, (2 * ROWS, ROWS), 0)
    r_in = lax.broadcasted_iota(i32, (2 * ROWS, ROWS), 1)
    before = jnp.where(r_out < ROWS, (r_in < r_out).astype(f32), (r_in == r_out - ROWS).astype(f32))
    nt = (((1,), (1,)), ((), ()))
    nn = (((1,), (0,)), ((), ()))
    column = lax.dot_general(before.astype(bf16), pairs, nt, preferred_element_type=f32)
    spot = lax.broadcasted_iota(i32, (ROWS, LIST_SPAN), 1).astype(f32)
    spot_row = lax.broadcasted_iota(i32, (1, LIST_SPAN), 1)
    p_row = lax.broadcasted_iota(i32, (PAIRS_MAX, LIST_SPAN), 0)
    for part, table_ref in ((0, local_table_ref), (1, halo_table_ref)):
        begin = column[0:ROWS, part:part + 1]
        end = begin + column[ROWS:2 * ROWS, part:part + 1]
        past = spot >= end
        inside = jnp.where((spot >= begin) & jnp.logical_not(past), f32(1), f32(0)).astype(bf16)
        past = jnp.where(past, f32(1), f32(0)).astype(bf16)
        pieces = piece_ref[part * 32:part * 32 + 32, :].astype(bf16)
        chosen = lax.dot_general(pieces, inside, nn, preferred_element_type=f32)
        ahead = lax.dot_general(pairs, past, nn, preferred_element_type=f32)[part:part + 1, :]
        ahead = ahead.astype(i32)
        mine = p_row == (spot_row - ahead)

        def field(at):
            return jnp.sum(
                jnp.where(mine, chosen[at:at + PAIRS_MAX, :], f32(0)), axis=0, keepdims=True
            ).astype(i32)

        place = field(0)
        item = (place & 15) | (chosen[24:25, :].astype(i32) << 4)
        item = item | (field(8) << 10) | (field(16) << 17) | ((place >> 4) << 24)
        for block in range(LIST_SPAN // 128):
            table_ref[block:block + 1, :] = item[:, block * 128:(block + 1) * 128]
        table_ref[TOTAL_ROW:TOTAL_ROW + 1, :] = ahead[:, LIST_SPAN - 128:LIST_SPAN]


def local_kernel(
    tiles_ref, cols_ref, count_ref, slab_ref,
    acc_ref, halo_ref, pre_ref,
    buf_ref, piece_ref, local_vmem, local_list, halo_list, load_sem, pre_sem, list_sem,
):
    build_lists(cols_ref, count_ref, piece_ref, halo_ref, local_vmem)
    to_local = pltpu.make_async_copy(local_vmem, local_list, list_sem.at[0])
    to_halo = pltpu.make_async_copy(halo_ref, halo_list, list_sem.at[1])
    to_local.start()
    to_halo.start()
    acc_ref[...] = jnp.zeros(acc_ref.shape, jnp.float32)
    to_local.wait()
    chunks = chunk_count(local_list)
    issue_first(local_list, 0, chunks, tiles_ref, buf_ref, load_sem)
    to_halo.wait()
    issue(halo_list, 0, tiles_ref, pre_ref, 0, pre_sem)
    run_chunks(local_list, 0, chunks, tiles_ref, buf_ref, load_sem, slab_ref, acc_ref)
    landed(tiles_ref, pre_ref, 0, pre_sem)


def halo_kernel(
    halo_list, tiles_ref, part_ref, pre_ref, arrived_ref, out_ref, buf_ref, slab_ref, acc_ref, load_sem
):
    chunks = chunk_count(halo_list)
    issue_first(halo_list, 1, chunks, tiles_ref, buf_ref, load_sem)
    acc_ref[...] = part_ref[...]
    slab_ref[0] = jnp.zeros(slab_ref.shape[1:], slab_ref.dtype)
    for s in range(ROWS):
        slab_ref[s + 1] = arrived_ref[s]
    add_chunk(halo_list, 0, pre_ref, 0, slab_ref, acc_ref)
    run_chunks(halo_list, 1, chunks, tiles_ref, buf_ref, load_sem, slab_ref, acc_ref)
    owners = out_ref.shape[0]
    each = ROWS // owners
    for owner in range(owners):
        for j in range(each):
            out_ref[owner, :, j * EDGE:(j + 1) * EDGE] = acc_ref[owner * each + j].astype(out_ref.dtype)


def per_device(features, tiles, tile_cols, tile_count, send_list, weight, bias):
    block_count, tile_depth, edge, _ = tiles.shape
    width = features.shape[1]
    feat_count = lax.axis_size("feat")
    vert_count = lax.axis_size("vert")
    bf16, f32, i32 = jnp.bfloat16, jnp.float32, jnp.int32
    whole = pl.BlockSpec(memory_space=VMEM)
    scalar = pl.BlockSpec(memory_space=SMEM)
    in_hbm = pl.BlockSpec(memory_space=pltpu.HBM)
    dma = pltpu.SemaphoreType.DMA
    mib = 1024 * 1024

    chosen, slabs, cols, counts = pl.pallas_call(
        pick_kernel,
        out_shape=(
            jax.ShapeDtypeStruct((block_count, width, edge), bf16),
            VMEM((SLOTS, width, edge), bf16),
            VMEM((tile_depth, block_count), i32),
            VMEM((1, block_count), i32),
        ),
        in_specs=[scalar, in_hbm, in_hbm, in_hbm],
        out_specs=(whole,) * 4,
        scratch_shapes=[VMEM((width, block_count * edge), bf16), dma((3,))],
        name="pick",
        cost_estimate=pl.CostEstimate(flops=1000, bytes_accessed=500000, transcendentals=0),
    )(send_list[0].T, features.T, tile_cols.T, tile_count.reshape(1, block_count))
    arrived = lax.all_to_all(
        chosen.reshape(vert_count, -1, width, edge), "vert", split_axis=0, concat_axis=0, tiled=True
    ).reshape(block_count, width, edge)

    flat_tiles = tiles.reshape(block_count * tile_depth, edge, edge)
    buffer = VMEM((2 * UNROLL * CHUNKS_MAX, edge, edge), bf16)
    part, halo, pre = pl.pallas_call(
        local_kernel,
        out_shape=(
            VMEM((block_count, width, edge), f32),
            VMEM((LIST_ROWS, 128), i32),
            VMEM((2 * UNROLL, edge, edge), bf16),
        ),
        in_specs=[in_hbm, whole, whole, whole],
        out_specs=(whole, whole, whole),
        scratch_shapes=[
            buffer,
            VMEM((72, block_count), f32),
            VMEM((LIST_ROWS, 128), i32),
            SMEM((LIST_ROWS, 128), i32),
            SMEM((LIST_ROWS, 128), i32),
            dma((CHUNKS_MAX,)),
            dma,
            dma((2,)),
        ],
        name="local",
        compiler_params=pltpu.CompilerParams(vmem_limit_bytes=44 * mib),
        cost_estimate=pl.CostEstimate(
            flops=8_000_000_000, bytes_accessed=17_000_000, transcendentals=0
        ),
    )(flat_tiles, cols, counts, slabs)

    hidden = pl.pallas_call(
        halo_kernel,
        out_shape=jax.ShapeDtypeStruct((feat_count, width, block_count * edge // feat_count), bf16),
        in_specs=[scalar, in_hbm, whole, whole, whole],
        out_specs=whole,
        scratch_shapes=[
            buffer,
            VMEM((SLOTS, width, edge), bf16),
            VMEM((block_count, width, edge), f32),
            dma((CHUNKS_MAX,)),
        ],
        name="halo",
        compiler_params=pltpu.CompilerParams(vmem_limit_bytes=44 * mib),
        cost_estimate=pl.CostEstimate(
            flops=3_000_000_000, bytes_accessed=17_000_000, transcendentals=0
        ),
    )(halo, flat_tiles, part, pre, arrived)

    full_rows = lax.all_to_all(hidden, "feat", split_axis=0, concat_axis=0, tiled=True)
    full_rows = full_rows.reshape(feat_count * width, -1)
    mixed_rows = lax.dot_general(
        full_rows, weight, (((0,), (0,)), ((), ())), preferred_element_type=f32
    )
    return jnp.maximum(mixed_rows + bias, f32(0.0)).astype(bf16)


def solution(mesh):
    return jax.shard_map(
        per_device,
        mesh=mesh,
        in_specs=(
            P("vert", "feat"),
            P("vert", None, None, None),
            P("vert", None),
            P("vert"),
            P("vert", None, None),
            P(),
            P(),
        ),
        out_specs=P(("vert", "feat"), None),
        check_vma=False,
    )
```

```python
import jax
import jax.numpy as jnp
from jax import lax
from jax.experimental import pallas as pl
from jax.experimental.pallas import tpu as pltpu
from jax.sharding import PartitionSpec as P

VMEM = pltpu.VMEM
SMEM = pltpu.SMEM
UNROLL = 32
PAIRS_MAX = 8
ROWS = 64
EDGE = 128
SLOTS = 2 * ROWS + 1
LIST_ROWS = 8
LIST_SPAN = 5 * 128
TOTAL_ROW = 5


def build_list(cols_ref, count_ref, piece_ref, table_ref):
    f32, i32, bf16 = jnp.float32, jnp.int32, jnp.bfloat16
    counts = count_ref[...]
    lane_row = lax.broadcasted_iota(i32, (1, ROWS), 1)
    for p in range(PAIRS_MAX):
        for half in range(2):
            k = 2 * p + half
            slot = jnp.where(counts > k, cols_ref[k:k + 1, :] + 1, 0)
            piece_ref[8 * half + p:8 * half + p + 1, :] = slot.astype(f32)
    piece_ref[16:17, :] = lane_row.astype(f32)
    piece_ref[17:24, :] = jnp.zeros((7, ROWS), f32)
    piece_ref[24:25, :] = ((counts + 1) >> 1).astype(f32)
    piece_ref[25:32, :] = jnp.zeros((7, ROWS), f32)

    pairs = piece_ref[24:32, :].astype(bf16)
    r_out = lax.broadcasted_iota(i32, (2 * ROWS, ROWS), 0)
    r_in = lax.broadcasted_iota(i32, (2 * ROWS, ROWS), 1)
    before = jnp.where(r_out < ROWS, (r_in < r_out).astype(f32), (r_in == r_out - ROWS).astype(f32))
    nt = (((1,), (1,)), ((), ()))
    nn = (((1,), (0,)), ((), ()))
    column = lax.dot_general(before.astype(bf16), pairs, nt, preferred_element_type=f32)
    spot = lax.broadcasted_iota(i32, (ROWS, LIST_SPAN), 1).astype(f32)
    spot_row = lax.broadcasted_iota(i32, (1, LIST_SPAN), 1)
    p_row = lax.broadcasted_iota(i32, (PAIRS_MAX, LIST_SPAN), 0)
    begin = column[0:ROWS, 0:1]
    end = begin + column[ROWS:2 * ROWS, 0:1]
    past = spot >= end
    inside = jnp.where((spot >= begin) & jnp.logical_not(past), f32(1), f32(0)).astype(bf16)
    past = jnp.where(past, f32(1), f32(0)).astype(bf16)
    pieces = piece_ref[0:24, :].astype(bf16)
    chosen = lax.dot_general(pieces, inside, nn, preferred_element_type=f32)
    ahead = lax.dot_general(pairs, past, nn, preferred_element_type=f32)[0:1, :].astype(i32)
    pair = spot_row - ahead
    mine = p_row == pair

    def field(at):
        return jnp.sum(
            jnp.where(mine, chosen[at:at + PAIRS_MAX, :], f32(0)), axis=0, keepdims=True
        ).astype(i32)

    item = (chosen[16:17, :].astype(i32) << 3) | (field(0) << 9) | (field(8) << 17)
    total = ahead[:, LIST_SPAN - 1:LIST_SPAN]
    item = jnp.where(spot_row < total, item | pair, 0)
    for block in range(LIST_SPAN // 128):
        table_ref[block:block + 1, :] = item[:, block * 128:(block + 1) * 128]
    table_ref[TOTAL_ROW:TOTAL_ROW + 1, :] = ahead[:, LIST_SPAN - 128:LIST_SPAN]


def pick_kernel(
    send_ref, feat_hbm, cols_hbm, count_hbm, out_ref, slab_ref, table_ref,
    feat_ref, cols_ref, count_ref, piece_ref, sem,
):
    copies = [
        pltpu.make_async_copy(src, dst, sem.at[i])
        for i, (src, dst) in enumerate(
            [(feat_hbm, feat_ref), (cols_hbm, cols_ref), (count_hbm, count_ref)]
        )
    ]
    for copy in copies:
        copy.start()
    copies[1].wait()
    copies[2].wait()
    build_list(cols_ref, count_ref, piece_ref, table_ref)
    copies[0].wait()
    slots, peers = send_ref.shape
    for peer in range(peers):
        for slot in range(slots):
            start = pl.multiple_of(send_ref[slot, peer] * EDGE, EDGE)
            out_ref[peer * slots + slot] = feat_ref[:, pl.ds(start, EDGE)]
    for r in range(ROWS):
        slab_ref[r] = feat_ref[:, r * EDGE:(r + 1) * EDGE]


def multiply_kernel(list_ref, tiles_ref, own_ref, arrived_ref, out_ref, slab_ref, acc_ref):
    acc_ref[...] = jnp.zeros(acc_ref.shape, jnp.float32)
    slab_ref[0] = jnp.zeros(slab_ref.shape[1:], slab_ref.dtype)
    slab_ref[1:ROWS + 1] = own_ref[...]
    slab_ref[ROWS + 1:] = arrived_ref[...]

    def chunk(i, carry):
        for u in range(UNROLL):
            at = i * UNROLL + u
            item = list_ref[at >> 7, at & 127]
            both = item & 511
            row = (item >> 3) & 63
            xa = (item >> 9) & 255
            xb = item >> 17
            tile = jnp.concatenate([tiles_ref[2 * both], tiles_ref[2 * both + 1]], axis=1)
            slab = jnp.concatenate([slab_ref[xa], slab_ref[xb]], axis=1)
            acc_ref[row] += lax.dot_general(
                slab, tile, (((1,), (1,)), ((), ())), preferred_element_type=jnp.float32
            )
        return carry

    lax.fori_loop(0, (list_ref[TOTAL_ROW, 127] + (UNROLL - 1)) // UNROLL, chunk, 0)
    owners = out_ref.shape[0]
    each = ROWS // owners
    for owner in range(owners):
        for j in range(each):
            out_ref[owner, :, j * EDGE:(j + 1) * EDGE] = acc_ref[owner * each + j].astype(out_ref.dtype)


def per_device(features, tiles, tile_cols, tile_count, send_list, weight, bias):
    block_count, tile_depth, edge, _ = tiles.shape
    width = features.shape[1]
    feat_count = lax.axis_size("feat")
    vert_count = lax.axis_size("vert")
    bf16, f32, i32 = jnp.bfloat16, jnp.float32, jnp.int32
    whole = pl.BlockSpec(memory_space=VMEM)
    scalar = pl.BlockSpec(memory_space=SMEM)
    in_hbm = pl.BlockSpec(memory_space=pltpu.HBM)
    dma = pltpu.SemaphoreType.DMA
    mib = 1024 * 1024

    def stay(x):
        return pltpu.with_memory_space_constraint(x, pltpu.HBM)

    flat_tiles = pltpu.with_memory_space_constraint(
        tiles.reshape(block_count * tile_depth, edge, edge), VMEM
    )

    chosen, slabs, table = pl.pallas_call(
        pick_kernel,
        out_shape=(
            VMEM((block_count, width, edge), bf16),
            VMEM((block_count, width, edge), bf16),
            VMEM((LIST_ROWS, 128), i32),
        ),
        in_specs=[scalar, in_hbm, in_hbm, in_hbm],
        out_specs=(whole,) * 3,
        scratch_shapes=[
            VMEM((width, block_count * edge), bf16),
            VMEM((tile_depth, block_count), i32),
            VMEM((1, block_count), i32),
            VMEM((32, block_count), f32),
            dma((3,)),
        ],
        name="pick",
        compiler_params=pltpu.CompilerParams(vmem_limit_bytes=4 * mib),
        cost_estimate=pl.CostEstimate(flops=20_000_000_000, bytes_accessed=200_000_000, transcendentals=0),
    )(
        stay(send_list[0].T), stay(features.T), stay(tile_cols.T),
        stay(tile_count.reshape(1, block_count)),
    )
    arrived = lax.all_to_all(
        chosen.reshape(vert_count, -1, width, edge), "vert", split_axis=0, concat_axis=0, tiled=True
    ).reshape(block_count, width, edge)

    hidden = pl.pallas_call(
        multiply_kernel,
        out_shape=jax.ShapeDtypeStruct((feat_count, width, block_count * edge // feat_count), bf16),
        in_specs=[scalar, whole, whole, whole],
        out_specs=whole,
        scratch_shapes=[
            VMEM((SLOTS, width, edge), bf16),
            VMEM((block_count, width, edge), f32),
        ],
        name="multiply",
        compiler_params=pltpu.CompilerParams(vmem_limit_bytes=8 * mib),
        cost_estimate=pl.CostEstimate(
            flops=8_000_000_000, bytes_accessed=17_000_000, transcendentals=0
        ),
    )(table, flat_tiles, slabs, arrived)

    full_rows = lax.all_to_all(hidden, "feat", split_axis=0, concat_axis=0, tiled=True)
    full_rows = full_rows.reshape(feat_count * width, -1)
    mixed_rows = lax.dot_general(
        full_rows, weight, (((0,), (0,)), ((), ())), preferred_element_type=f32
    )
    return jnp.maximum(mixed_rows + bias, f32(0.0)).astype(bf16)


def solution(mesh):
    return jax.shard_map(
        per_device,
        mesh=mesh,
        in_specs=(
            P("vert", "feat"),
            P("vert", None, None, None),
            P("vert", None),
            P("vert"),
            P("vert", None, None),
            P(),
            P(),
        ),
        out_specs=P(("vert", "feat"), None),
        check_vma=False,
    )
```

```python
import jax
import jax.numpy as jnp
from jax import lax
from jax.experimental import pallas as pl
from jax.experimental.pallas import tpu as pltpu
from jax.sharding import PartitionSpec as P

VMEM = pltpu.VMEM
SMEM = pltpu.SMEM
EACH = 24
PAIRS_MAX = 8
ROWS = 64
HALF = ROWS // 2
EDGE = 128
SLOTS = 2 * ROWS + 1
LIST_ROWS = 8
LIST_BLOCKS = 3
LIST_SPAN = LIST_BLOCKS * 128
LENGTH_ROW = 2 * LIST_BLOCKS


def build_list(cols_ref, count_ref, piece_ref, table_ref):
    f32, i32, bf16 = jnp.float32, jnp.int32, jnp.bfloat16
    counts = count_ref[...]
    lane_row = lax.broadcasted_iota(i32, (1, ROWS), 1)
    for p in range(PAIRS_MAX):
        for half in range(2):
            k = 2 * p + half
            slot = jnp.where(counts > k, cols_ref[k:k + 1, :] + 1, 0)
            piece_ref[8 * half + p:8 * half + p + 1, :] = slot.astype(f32)
    piece_ref[16:17, :] = lane_row.astype(f32)
    piece_ref[17:24, :] = jnp.zeros((7, ROWS), f32)
    pairs_each = ((counts + 1) >> 1).astype(f32)
    odd = lane_row & 1
    for part in range(2):
        piece_ref[24 + part:25 + part, :] = jnp.where(odd == part, pairs_each, f32(0))
    piece_ref[26:32, :] = jnp.zeros((6, ROWS), f32)

    pairs = piece_ref[24:32, :].astype(bf16)
    r_out = lax.broadcasted_iota(i32, (2 * ROWS, ROWS), 0)
    r_in = lax.broadcasted_iota(i32, (2 * ROWS, ROWS), 1)
    before = jnp.where(r_out < ROWS, (r_in < r_out).astype(f32), (r_in == r_out - ROWS).astype(f32))
    nt = (((1,), (1,)), ((), ()))
    nn = (((1,), (0,)), ((), ()))
    column = lax.dot_general(before.astype(bf16), pairs, nt, preferred_element_type=f32)
    spot = lax.broadcasted_iota(i32, (ROWS, LIST_SPAN), 1).astype(f32)
    spot_row = lax.broadcasted_iota(i32, (1, LIST_SPAN), 1)
    p_row = lax.broadcasted_iota(i32, (PAIRS_MAX, LIST_SPAN), 0)
    pieces = piece_ref[0:24, :].astype(bf16)
    for part in range(2):
        begin = column[0:ROWS, part:part + 1]
        end = begin + column[ROWS:2 * ROWS, part:part + 1]
        past = spot >= end
        inside = jnp.where((spot >= begin) & jnp.logical_not(past), f32(1), f32(0)).astype(bf16)
        past = jnp.where(past, f32(1), f32(0)).astype(bf16)
        chosen = lax.dot_general(pieces, inside, nn, preferred_element_type=f32)
        ahead = lax.dot_general(pairs, past, nn, preferred_element_type=f32)
        ahead = ahead[part:part + 1, :].astype(i32)
        pair = spot_row - ahead
        mine = p_row == pair

        def field(at):
            return jnp.sum(
                jnp.where(mine, chosen[at:at + PAIRS_MAX, :], f32(0)), axis=0, keepdims=True
            ).astype(i32)

        item = (chosen[16:17, :].astype(i32) << 3) | (field(0) << 9) | (field(8) << 17)
        total = ahead[:, LIST_SPAN - 1:LIST_SPAN]
        item = jnp.where(spot_row < total, item | pair, 0)
        for block in range(LIST_BLOCKS):
            at = part * LIST_BLOCKS + block
            table_ref[at:at + 1, :] = item[:, block * 128:(block + 1) * 128]
        at = LENGTH_ROW + part
        table_ref[at:at + 1, :] = ahead[:, LIST_SPAN - 128:LIST_SPAN]


def pick_kernel(
    send_hbm, feat_hbm, cols_hbm, count_hbm, out_ref, slab_ref, table_ref,
    send_ref, feat_ref, cols_ref, count_ref, piece_ref, sem,
):
    copies = [
        pltpu.make_async_copy(src, dst, sem.at[i])
        for i, (src, dst) in enumerate(
            [(feat_hbm, feat_ref), (cols_hbm, cols_ref), (count_hbm, count_ref), (send_hbm, send_ref)]
        )
    ]
    for copy in copies:
        copy.start()
    copies[1].wait()
    copies[2].wait()
    build_list(cols_ref, count_ref, piece_ref, table_ref)
    copies[3].wait()
    copies[0].wait()
    slots, peers = send_ref.shape
    for peer in range(peers):
        for slot in range(slots):
            start = pl.multiple_of(send_ref[slot, peer] * EDGE, EDGE)
            out_ref[peer * slots + slot] = feat_ref[:, pl.ds(start, EDGE)]
    for r in range(ROWS):
        slab_ref[r] = feat_ref[:, r * EDGE:(r + 1) * EDGE]


def multiply_kernel(
    table_ref, tiles_ref, own_ref, arrived_ref, out_ref, list_ref, slab_ref, even_ref, odd_ref, sem
):
    to_smem = pltpu.make_async_copy(table_ref, list_ref, sem)
    to_smem.start()
    even_ref[...] = jnp.zeros(even_ref.shape, jnp.float32)
    odd_ref[...] = jnp.zeros(odd_ref.shape, jnp.float32)
    slab_ref[0] = jnp.zeros(slab_ref.shape[1:], slab_ref.dtype)
    slab_ref[1:ROWS + 1] = own_ref[...]
    slab_ref[ROWS + 1:] = arrived_ref[...]
    to_smem.wait()
    contract = (((1,), (1,)), ((), ()))

    def add_pair(part, at):
        item = list_ref[part * LIST_BLOCKS + (at >> 7), at & 127]
        both = item & 511
        row = (item >> 4) & 31
        tile = jnp.concatenate([tiles_ref[2 * both], tiles_ref[2 * both + 1]], axis=1)
        slab = jnp.concatenate([slab_ref[(item >> 9) & 255], slab_ref[item >> 17]], axis=1)
        if part == 0:
            even_ref[row] += lax.dot_general(tile, slab, contract, preferred_element_type=jnp.float32)
        else:
            odd_ref[row] += lax.dot_general(slab, tile, contract, preferred_element_type=jnp.float32)

    def chunk(i, carry):
        for u in range(0, EACH, 2):
            for part in range(2):
                for v in range(2):
                    add_pair(part, i * EACH + u + v)
        return carry

    longest = jnp.maximum(list_ref[LENGTH_ROW, 127], list_ref[LENGTH_ROW + 1, 127])
    lax.fori_loop(0, (longest + (EACH - 1)) // EACH, chunk, 0)
    owners = out_ref.shape[0]
    each = ROWS // owners
    for row in range(HALF):
        owner, j = divmod(2 * row, each)
        out_ref[owner, :, j * EDGE:(j + 1) * EDGE] = even_ref[row].astype(out_ref.dtype).T
        out_ref[owner, :, (j + 1) * EDGE:(j + 2) * EDGE] = odd_ref[row].astype(out_ref.dtype)


def per_device(features, tiles, tile_cols, tile_count, send_list, weight, bias):
    block_count, tile_depth, edge, _ = tiles.shape
    width = features.shape[1]
    feat_count = lax.axis_size("feat")
    vert_count = lax.axis_size("vert")
    bf16, f32, i32 = jnp.bfloat16, jnp.float32, jnp.int32
    whole = pl.BlockSpec(memory_space=VMEM)
    in_hbm = pl.BlockSpec(memory_space=pltpu.HBM)
    dma = pltpu.SemaphoreType.DMA
    mib = 1024 * 1024

    def stay(x):
        return pltpu.with_memory_space_constraint(x, pltpu.HBM)

    flat_tiles = pltpu.with_memory_space_constraint(
        tiles.reshape(block_count * tile_depth, edge, edge), VMEM
    )

    chosen, slabs, table = pl.pallas_call(
        pick_kernel,
        out_shape=(
            VMEM((block_count, width, edge), bf16),
            VMEM((block_count, width, edge), bf16),
            VMEM((LIST_ROWS, 128), i32),
        ),
        in_specs=[in_hbm] * 4,
        out_specs=(whole,) * 3,
        scratch_shapes=[
            SMEM(send_list.shape[:0:-1], i32),
            VMEM((width, block_count * edge), bf16),
            VMEM((tile_depth, block_count), i32),
            VMEM((1, block_count), i32),
            VMEM((32, block_count), f32),
            dma((4,)),
        ],
        name="pick",
        compiler_params=pltpu.CompilerParams(vmem_limit_bytes=4 * mib),
        cost_estimate=pl.CostEstimate(flops=20_000_000_000, bytes_accessed=200_000_000, transcendentals=0),
    )(
        stay(send_list[0].T), stay(features.T), stay(tile_cols.T),
        stay(tile_count.reshape(1, block_count)),
    )
    arrived = lax.all_to_all(
        chosen.reshape(vert_count, -1, width, edge), "vert", split_axis=0, concat_axis=0, tiled=True
    ).reshape(block_count, width, edge)

    hidden = pl.pallas_call(
        multiply_kernel,
        out_shape=jax.ShapeDtypeStruct((feat_count, width, block_count * edge // feat_count), bf16),
        in_specs=[whole, whole, whole, whole],
        out_specs=whole,
        scratch_shapes=[
            SMEM((LIST_ROWS, 128), i32),
            VMEM((SLOTS, width, edge), bf16),
            VMEM((HALF, edge, width), f32),
            VMEM((HALF, width, edge), f32),
            dma,
        ],
        name="multiply",
        compiler_params=pltpu.CompilerParams(vmem_limit_bytes=8 * mib),
        cost_estimate=pl.CostEstimate(
            flops=8_000_000_000, bytes_accessed=17_000_000, transcendentals=0
        ),
    )(table, flat_tiles, slabs, arrived)

    full_rows = lax.all_to_all(hidden, "feat", split_axis=0, concat_axis=0, tiled=True)
    full_rows = full_rows.reshape(feat_count * width, -1)
    mixed_rows = lax.dot_general(
        full_rows, weight, (((0,), (0,)), ((), ())), preferred_element_type=f32
    )
    return jnp.maximum(mixed_rows + bias, f32(0.0)).astype(bf16)


def solution(mesh):
    return jax.shard_map(
        per_device,
        mesh=mesh,
        in_specs=(
            P("vert", "feat"),
            P("vert", None, None, None),
            P("vert", None),
            P("vert"),
            P("vert", None, None),
            P(),
            P(),
        ),
        out_specs=P(("vert", "feat"), None),
        check_vma=False,
    )
```

```python
import jax
import jax.numpy as jnp
from jax import lax
from jax.experimental import pallas as pl
from jax.experimental.pallas import tpu as pltpu
from jax.sharding import PartitionSpec as P

VMEM = pltpu.VMEM
SMEM = pltpu.SMEM
EACH = 32
PAIRS_MAX = 8
ROWS = 64
HALF = ROWS // 2
EDGE = 128
SLOTS = 2 * ROWS + 1
LIST_ROWS = 8
LIST_BLOCKS = 3
LIST_SPAN = LIST_BLOCKS * 128
LENGTH_ROW = 2 * LIST_BLOCKS


def build_list(cols_ref, count_ref, piece_ref, table_ref):
    f32, i32, bf16 = jnp.float32, jnp.int32, jnp.bfloat16
    counts = count_ref[...]
    lane_row = lax.broadcasted_iota(i32, (1, ROWS), 1)
    for p in range(PAIRS_MAX):
        for half in range(2):
            k = 2 * p + half
            slot = jnp.where(counts > k, cols_ref[k:k + 1, :] + 1, 0)
            piece_ref[8 * half + p:8 * half + p + 1, :] = slot.astype(f32)
    piece_ref[16:17, :] = lane_row.astype(f32)
    piece_ref[17:24, :] = jnp.zeros((7, ROWS), f32)
    pairs_each = ((counts + 1) >> 1).astype(f32)
    odd = lane_row & 1
    for part in range(2):
        piece_ref[24 + part:25 + part, :] = jnp.where(odd == part, pairs_each, f32(0))
    piece_ref[26:32, :] = jnp.zeros((6, ROWS), f32)

    pairs = piece_ref[24:32, :].astype(bf16)
    r_out = lax.broadcasted_iota(i32, (2 * ROWS, ROWS), 0)
    r_in = lax.broadcasted_iota(i32, (2 * ROWS, ROWS), 1)
    before = jnp.where(r_out < ROWS, (r_in < r_out).astype(f32), (r_in == r_out - ROWS).astype(f32))
    nt = (((1,), (1,)), ((), ()))
    nn = (((1,), (0,)), ((), ()))
    column = lax.dot_general(before.astype(bf16), pairs, nt, preferred_element_type=f32)
    spot = lax.broadcasted_iota(i32, (ROWS, LIST_SPAN), 1).astype(f32)
    spot_row = lax.broadcasted_iota(i32, (1, LIST_SPAN), 1)
    p_row = lax.broadcasted_iota(i32, (PAIRS_MAX, LIST_SPAN), 0)
    pieces = piece_ref[0:24, :].astype(bf16)
    for part in range(2):
        begin = column[0:ROWS, part:part + 1]
        end = begin + column[ROWS:2 * ROWS, part:part + 1]
        past = spot >= end
        inside = jnp.where((spot >= begin) & jnp.logical_not(past), f32(1), f32(0)).astype(bf16)
        past = jnp.where(past, f32(1), f32(0)).astype(bf16)
        chosen = lax.dot_general(pieces, inside, nn, preferred_element_type=f32)
        ahead = lax.dot_general(pairs, past, nn, preferred_element_type=f32)
        ahead = ahead[part:part + 1, :].astype(i32)
        pair = spot_row - ahead
        mine = p_row == pair

        def field(at):
            return jnp.sum(
                jnp.where(mine, chosen[at:at + PAIRS_MAX, :], f32(0)), axis=0, keepdims=True
            ).astype(i32)

        item = (chosen[16:17, :].astype(i32) << 3) | (field(0) << 9) | (field(8) << 17)
        total = ahead[:, LIST_SPAN - 1:LIST_SPAN]
        item = jnp.where(spot_row < total, item | pair, 0)
        for block in range(LIST_BLOCKS):
            at = part * LIST_BLOCKS + block
            table_ref[at:at + 1, :] = item[:, block * 128:(block + 1) * 128]
        at = LENGTH_ROW + part
        table_ref[at:at + 1, :] = ahead[:, LIST_SPAN - 128:LIST_SPAN]


def pick_kernel(
    send_hbm, feat_hbm, cols_hbm, count_hbm, out_ref, slab_ref, list_ref,
    send_ref, feat_ref, cols_ref, count_ref, piece_ref, table_ref, sem,
):
    copies = [
        pltpu.make_async_copy(src, dst, sem.at[i])
        for i, (src, dst) in enumerate(
            [(feat_hbm, feat_ref), (cols_hbm, cols_ref), (count_hbm, count_ref), (send_hbm, send_ref)]
        )
    ]
    for copy in copies:
        copy.start()
    copies[1].wait()
    copies[2].wait()
    build_list(cols_ref, count_ref, piece_ref, table_ref)
    to_smem = pltpu.make_async_copy(table_ref, list_ref, sem.at[4])
    to_smem.start()
    copies[3].wait()
    copies[0].wait()
    slots, peers = send_ref.shape
    for peer in range(peers):
        for slot in range(slots):
            start = pl.multiple_of(send_ref[slot, peer] * EDGE, EDGE)
            out_ref[peer * slots + slot] = feat_ref[:, pl.ds(start, EDGE)]
    for r in range(ROWS):
        slab_ref[r] = feat_ref[:, r * EDGE:(r + 1) * EDGE]
    to_smem.wait()


def multiply_kernel(
    list_ref, tiles_ref, own_ref, arrived_ref, out_ref, slab_ref, even_ref, odd_ref
):
    even_ref[...] = jnp.zeros(even_ref.shape, jnp.float32)
    odd_ref[...] = jnp.zeros(odd_ref.shape, jnp.float32)
    slab_ref[0] = jnp.zeros(slab_ref.shape[1:], slab_ref.dtype)
    slab_ref[1:ROWS + 1] = own_ref[...]
    slab_ref[ROWS + 1:] = arrived_ref[...]
    contract = (((1,), (1,)), ((), ()))

    def add_pair(part, at):
        item = list_ref[part * LIST_BLOCKS + (at >> 7), at & 127]
        both = item & 511
        row = (item >> 4) & 31
        tile = jnp.concatenate([tiles_ref[2 * both], tiles_ref[2 * both + 1]], axis=1)
        slab = jnp.concatenate([slab_ref[(item >> 9) & 255], slab_ref[item >> 17]], axis=1)
        if part == 0:
            even_ref[row] += lax.dot_general(tile, slab, contract, preferred_element_type=jnp.float32)
        else:
            odd_ref[row] += lax.dot_general(slab, tile, contract, preferred_element_type=jnp.float32)

    def chunk(i, carry):
        for u in range(0, EACH, 2):
            for part in range(2):
                for v in range(2):
                    add_pair(part, i * EACH + u + v)
        return carry

    longest = jnp.maximum(list_ref[LENGTH_ROW, 127], list_ref[LENGTH_ROW + 1, 127])
    lax.fori_loop(0, (longest + (EACH - 1)) // EACH, chunk, 0)
    owners = out_ref.shape[0]
    each = ROWS // owners
    for row in range(HALF):
        owner, j = divmod(2 * row, each)
        out_ref[owner, :, j * EDGE:(j + 1) * EDGE] = even_ref[row].astype(out_ref.dtype).T
        out_ref[owner, :, (j + 1) * EDGE:(j + 2) * EDGE] = odd_ref[row].astype(out_ref.dtype)


def per_device(features, tiles, tile_cols, tile_count, send_list, weight, bias):
    block_count, tile_depth, edge, _ = tiles.shape
    width = features.shape[1]
    feat_count = lax.axis_size("feat")
    vert_count = lax.axis_size("vert")
    bf16, f32, i32 = jnp.bfloat16, jnp.float32, jnp.int32
    whole = pl.BlockSpec(memory_space=VMEM)
    scalar = pl.BlockSpec(memory_space=SMEM)
    in_hbm = pl.BlockSpec(memory_space=pltpu.HBM)
    dma = pltpu.SemaphoreType.DMA
    mib = 1024 * 1024

    def stay(x):
        return pltpu.with_memory_space_constraint(x, pltpu.HBM)

    flat_tiles = pltpu.with_memory_space_constraint(
        tiles.reshape(block_count * tile_depth, edge, edge), VMEM
    )

    chosen, slabs, table = pl.pallas_call(
        pick_kernel,
        out_shape=(
            VMEM((block_count, width, edge), bf16),
            VMEM((block_count, width, edge), bf16),
            SMEM((LIST_ROWS, 128), i32),
        ),
        in_specs=[in_hbm] * 4,
        out_specs=(whole, whole, scalar),
        scratch_shapes=[
            SMEM(send_list.shape[:0:-1], i32),
            VMEM((width, block_count * edge), bf16),
            VMEM((tile_depth, block_count), i32),
            VMEM((1, block_count), i32),
            VMEM((32, block_count), f32),
            VMEM((LIST_ROWS, 128), i32),
            dma((5,)),
        ],
        name="pick",
        compiler_params=pltpu.CompilerParams(vmem_limit_bytes=4 * mib),
        cost_estimate=pl.CostEstimate(flops=20_000_000_000, bytes_accessed=200_000_000, transcendentals=0),
    )(
        stay(send_list[0].T), stay(features.T), stay(tile_cols.T),
        stay(tile_count.reshape(1, block_count)),
    )
    arrived = lax.all_to_all(
        chosen.reshape(vert_count, -1, width, edge), "vert", split_axis=0, concat_axis=0, tiled=True
    ).reshape(block_count, width, edge)

    hidden = pl.pallas_call(
        multiply_kernel,
        out_shape=jax.ShapeDtypeStruct((feat_count, width, block_count * edge // feat_count), bf16),
        in_specs=[scalar, whole, whole, whole],
        out_specs=whole,
        scratch_shapes=[
            VMEM((SLOTS, width, edge), bf16),
            VMEM((HALF, edge, width), f32),
            VMEM((HALF, width, edge), f32),
        ],
        name="multiply",
        compiler_params=pltpu.CompilerParams(vmem_limit_bytes=8 * mib),
        cost_estimate=pl.CostEstimate(
            flops=8_000_000_000, bytes_accessed=17_000_000, transcendentals=0
        ),
    )(table, flat_tiles, slabs, arrived)

    full_rows = lax.all_to_all(hidden, "feat", split_axis=0, concat_axis=0, tiled=True)
    full_rows = full_rows.reshape(feat_count * width, -1)
    mixed_rows = lax.dot_general(
        full_rows, weight, (((0,), (0,)), ((), ())), preferred_element_type=f32
    )
    return jnp.maximum(mixed_rows + bias, f32(0.0)).astype(bf16)


def solution(mesh):
    return jax.shard_map(
        per_device,
        mesh=mesh,
        in_specs=(
            P("vert", "feat"),
            P("vert", None, None, None),
            P("vert", None),
            P("vert"),
            P("vert", None, None),
            P(),
            P(),
        ),
        out_specs=P(("vert", "feat"), None),
        check_vma=False,
    )
```

```python
import jax
import jax.numpy as jnp
from jax import lax
from jax.experimental import pallas as pl
from jax.experimental.pallas import tpu as pltpu
from jax.sharding import PartitionSpec as P

VMEM = pltpu.VMEM
SMEM = pltpu.SMEM
EACH = 24
PAIRS_MAX = 8
ROWS = 64
HALF = ROWS // 2
EDGE = 128
SLOTS = 2 * ROWS + 1
LIST_ROWS = 8
LIST_BLOCKS = 2
LIST_SPAN = LIST_BLOCKS * 128
LENGTH_ROW = 2 * LIST_BLOCKS


def build_list(cols_ref, count_ref, piece_ref, table_ref):
    f32, i32, bf16 = jnp.float32, jnp.int32, jnp.bfloat16
    counts = count_ref[...]
    lane_row = lax.broadcasted_iota(i32, (1, ROWS), 1)
    for p in range(PAIRS_MAX):
        for half in range(2):
            k = 2 * p + half
            slot = jnp.where(counts > k, cols_ref[k:k + 1, :] + 1, 0)
            piece_ref[8 * half + p:8 * half + p + 1, :] = slot.astype(f32)
    piece_ref[16:17, :] = lane_row.astype(f32)
    piece_ref[17:24, :] = jnp.zeros((7, ROWS), f32)
    pairs_each = ((counts - 1) >> 1).astype(f32)
    odd = lane_row & 1
    for part in range(2):
        piece_ref[24 + part:25 + part, :] = jnp.where(odd == part, pairs_each, f32(0))
    piece_ref[26:32, :] = jnp.zeros((6, ROWS), f32)

    pairs = piece_ref[24:32, :].astype(bf16)
    r_out = lax.broadcasted_iota(i32, (2 * ROWS, ROWS), 0)
    r_in = lax.broadcasted_iota(i32, (2 * ROWS, ROWS), 1)
    before = jnp.where(r_out < ROWS, (r_in < r_out).astype(f32), (r_in == r_out - ROWS).astype(f32))
    nt = (((1,), (1,)), ((), ()))
    nn = (((1,), (0,)), ((), ()))
    column = lax.dot_general(before.astype(bf16), pairs, nt, preferred_element_type=f32)
    spot = lax.broadcasted_iota(i32, (ROWS, LIST_SPAN), 1).astype(f32)
    spot_row = lax.broadcasted_iota(i32, (1, LIST_SPAN), 1)
    p_row = lax.broadcasted_iota(i32, (PAIRS_MAX, LIST_SPAN), 0)
    pieces = piece_ref[0:24, :].astype(bf16)
    for part in range(2):
        begin = column[0:ROWS, part:part + 1]
        end = begin + column[ROWS:2 * ROWS, part:part + 1]
        past = spot >= end
        inside = jnp.where((spot >= begin) & jnp.logical_not(past), f32(1), f32(0)).astype(bf16)
        past = jnp.where(past, f32(1), f32(0)).astype(bf16)
        chosen = lax.dot_general(pieces, inside, nn, preferred_element_type=f32)
        ahead = lax.dot_general(pairs, past, nn, preferred_element_type=f32)
        ahead = ahead[part:part + 1, :].astype(i32)
        pair = spot_row - ahead + 1
        mine = p_row == pair

        def field(at):
            return jnp.sum(
                jnp.where(mine, chosen[at:at + PAIRS_MAX, :], f32(0)), axis=0, keepdims=True
            ).astype(i32)

        item = (chosen[16:17, :].astype(i32) << 3) | (field(0) << 9) | (field(8) << 17)
        total = ahead[:, LIST_SPAN - 1:LIST_SPAN]
        item = jnp.where(spot_row < total, item | pair, 0)
        for block in range(LIST_BLOCKS):
            at = part * LIST_BLOCKS + block
            table_ref[at:at + 1, :] = item[:, block * 128:(block + 1) * 128]
        at = LENGTH_ROW + part
        table_ref[at:at + 1, :] = ahead[:, LIST_SPAN - 128:LIST_SPAN]


def pick_kernel(
    send_hbm, feat_hbm, cols_hbm, count_hbm, out_ref, slab_ref, table_ref, cols_out, count_out,
    send_ref, feat_ref, cols_ref, count_ref, piece_ref, sem,
):
    copies = [
        pltpu.make_async_copy(src, dst, sem.at[i])
        for i, (src, dst) in enumerate([
            (feat_hbm, feat_ref), (cols_hbm, cols_ref), (count_hbm, count_ref), (send_hbm, send_ref),
            (cols_hbm, cols_out), (count_hbm, count_out),
        ])
    ]
    for copy in copies:
        copy.start()
    slab_ref[0] = jnp.zeros(slab_ref.shape[1:], slab_ref.dtype)
    copies[1].wait()
    copies[2].wait()
    build_list(cols_ref, count_ref, piece_ref, table_ref)
    copies[3].wait()
    copies[0].wait()
    slots, peers = send_ref.shape
    for peer in range(peers):
        for slot in range(slots):
            start = pl.multiple_of(send_ref[slot, peer] * EDGE, EDGE)
            out_ref[peer * slots + slot] = feat_ref[:, pl.ds(start, EDGE)]
    for r in range(ROWS):
        slab_ref[r + 1] = feat_ref[:, r * EDGE:(r + 1) * EDGE]
    copies[4].wait()
    copies[5].wait()


def multiply_kernel(
    cols_ref, count_ref, table_ref, tiles_ref, own_ref, arrived_ref, out_ref, slab_ref,
    list_ref, even_ref, odd_ref, sem,
):
    to_smem = pltpu.make_async_copy(table_ref, list_ref, sem)
    to_smem.start()
    slab_ref[ROWS + 1:] = arrived_ref[...]
    contract = (((1,), (1,)), ((), ()))

    def product(part, both, a, b):
        tile = jnp.concatenate([tiles_ref[2 * both], tiles_ref[2 * both + 1]], axis=1)
        slab = jnp.concatenate([slab_ref[a], slab_ref[b]], axis=1)
        left, right = (tile, slab) if part == 0 else (slab, tile)
        return lax.dot_general(left, right, contract, preferred_element_type=jnp.float32)

    sums = (even_ref, odd_ref)
    for first in range(0, ROWS, 4):
        for part in range(2):
            for row in (first + part, first + part + 2):
                a = cols_ref[0, row] + 1
                b = jnp.where(count_ref[0, row] > 1, cols_ref[1, row] + 1, 0)
                sums[part][row // 2] = product(part, row * PAIRS_MAX, a, b)
    to_smem.wait()

    def chunk(i, carry):
        for u in range(0, EACH, 2):
            for part in range(2):
                for v in range(2):
                    at = i * EACH + u + v
                    item = list_ref[part * LIST_BLOCKS + (at >> 7), at & 127]
                    sums[part][(item >> 4) & 31] += product(
                        part, item & 511, (item >> 9) & 255, item >> 17
                    )
        return carry

    longest = jnp.maximum(list_ref[LENGTH_ROW, 127], list_ref[LENGTH_ROW + 1, 127])
    lax.fori_loop(0, (longest + (EACH - 1)) // EACH, chunk, 0)
    owners = out_ref.shape[0]
    each = ROWS // owners
    for row in range(HALF):
        owner, j = divmod(2 * row, each)
        out_ref[owner, :, j * EDGE:(j + 1) * EDGE] = even_ref[row].astype(out_ref.dtype).T
        out_ref[owner, :, (j + 1) * EDGE:(j + 2) * EDGE] = odd_ref[row].astype(out_ref.dtype)


def per_device(features, tiles, tile_cols, tile_count, send_list, weight, bias):
    block_count, tile_depth, edge, _ = tiles.shape
    width = features.shape[1]
    feat_count = lax.axis_size("feat")
    vert_count = lax.axis_size("vert")
    bf16, f32, i32 = jnp.bfloat16, jnp.float32, jnp.int32
    whole = pl.BlockSpec(memory_space=VMEM)
    scalar = pl.BlockSpec(memory_space=SMEM)
    in_hbm = pl.BlockSpec(memory_space=pltpu.HBM)
    dma = pltpu.SemaphoreType.DMA
    mib = 1024 * 1024

    def stay(x):
        return pltpu.with_memory_space_constraint(x, pltpu.HBM)

    flat_tiles = pltpu.with_memory_space_constraint(
        tiles.reshape(block_count * tile_depth, edge, edge), VMEM
    )

    chosen, slabs, table, cols, counts = pl.pallas_call(
        pick_kernel,
        out_shape=(
            VMEM((block_count, width, edge), bf16),
            VMEM((SLOTS, width, edge), bf16),
            VMEM((LIST_ROWS, 128), i32),
            SMEM((tile_depth, block_count), i32),
            SMEM((1, block_count), i32),
        ),
        in_specs=[in_hbm] * 4,
        out_specs=(whole, whole, whole, scalar, scalar),
        scratch_shapes=[
            SMEM(send_list.shape[:0:-1], i32),
            VMEM((width, block_count * edge), bf16),
            VMEM((tile_depth, block_count), i32),
            VMEM((1, block_count), i32),
            VMEM((32, block_count), f32),
            dma((6,)),
        ],
        name="pick",
        compiler_params=pltpu.CompilerParams(vmem_limit_bytes=4 * mib),
        cost_estimate=pl.CostEstimate(flops=20_000_000_000, bytes_accessed=200_000_000, transcendentals=0),
    )(
        stay(send_list[0].T), stay(features.T), stay(tile_cols.T),
        stay(tile_count.reshape(1, block_count)),
    )
    arrived = lax.all_to_all(
        chosen.reshape(vert_count, -1, width, edge), "vert", split_axis=0, concat_axis=0, tiled=True
    ).reshape(block_count, width, edge)

    hidden, _ = pl.pallas_call(
        multiply_kernel,
        out_shape=(
            jax.ShapeDtypeStruct((feat_count, width, block_count * edge // feat_count), bf16),
            VMEM((SLOTS, width, edge), bf16),
        ),
        in_specs=[scalar, scalar, whole, whole, whole, whole],
        out_specs=(whole, whole),
        scratch_shapes=[
            SMEM((LIST_ROWS, 128), i32),
            VMEM((HALF, edge, width), f32),
            VMEM((HALF, width, edge), f32),
            dma,
        ],
        input_output_aliases={4: 1},
        name="multiply",
        compiler_params=pltpu.CompilerParams(vmem_limit_bytes=8 * mib),
        cost_estimate=pl.CostEstimate(
            flops=8_000_000_000, bytes_accessed=17_000_000, transcendentals=0
        ),
    )(cols, counts, table, flat_tiles, slabs, arrived)

    full_rows = lax.all_to_all(hidden, "feat", split_axis=0, concat_axis=0, tiled=True)
    full_rows = full_rows.reshape(feat_count * width, -1)
    mixed_rows = lax.dot_general(
        full_rows, weight, (((0,), (0,)), ((), ())), preferred_element_type=f32
    )
    return jnp.maximum(mixed_rows + bias, f32(0.0)).astype(bf16)


def solution(mesh):
    return jax.shard_map(
        per_device,
        mesh=mesh,
        in_specs=(
            P("vert", "feat"),
            P("vert", None, None, None),
            P("vert", None),
            P("vert"),
            P("vert", None, None),
            P(),
            P(),
        ),
        out_specs=P(("vert", "feat"), None),
        check_vma=False,
    )
```

```python
import jax
import jax.numpy as jnp
from jax import lax
from jax.experimental import pallas as pl
from jax.experimental.pallas import tpu as pltpu
from jax.sharding import PartitionSpec as P

VMEM = pltpu.VMEM
SMEM = pltpu.SMEM
EACH = 32
PAIRS_MAX = 8
ROWS = 64
HALF = ROWS // 2
EDGE = 128
SLOTS = 2 * ROWS + 1
LIST_ROWS = 8
LIST_BLOCKS = 2
LIST_SPAN = LIST_BLOCKS * 128
LENGTH_ROW = 2 * LIST_BLOCKS


def build_list(cols_ref, count_ref, piece_ref, table_ref):
    f32, i32, bf16 = jnp.float32, jnp.int32, jnp.bfloat16
    counts = count_ref[...]
    lane_row = lax.broadcasted_iota(i32, (1, ROWS), 1)
    for p in range(PAIRS_MAX):
        for half in range(2):
            k = 2 * p + half
            slot = jnp.where(counts > k, cols_ref[k:k + 1, :] + 1, 0)
            piece_ref[8 * half + p:8 * half + p + 1, :] = slot.astype(f32)
    piece_ref[16:17, :] = lane_row.astype(f32)
    piece_ref[17:24, :] = jnp.zeros((7, ROWS), f32)
    pairs_each = ((counts - 1) >> 1).astype(f32)
    odd = lane_row & 1
    for part in range(2):
        piece_ref[24 + part:25 + part, :] = jnp.where(odd == part, pairs_each, f32(0))
    piece_ref[26:32, :] = jnp.zeros((6, ROWS), f32)

    pairs = piece_ref[24:32, :].astype(bf16)
    r_out = lax.broadcasted_iota(i32, (2 * ROWS, ROWS), 0)
    r_in = lax.broadcasted_iota(i32, (2 * ROWS, ROWS), 1)
    before = jnp.where(r_out < ROWS, (r_in < r_out).astype(f32), (r_in == r_out - ROWS).astype(f32))
    nt = (((1,), (1,)), ((), ()))
    nn = (((1,), (0,)), ((), ()))
    column = lax.dot_general(before.astype(bf16), pairs, nt, preferred_element_type=f32)
    spot = lax.broadcasted_iota(i32, (ROWS, LIST_SPAN), 1).astype(f32)
    spot_row = lax.broadcasted_iota(i32, (1, LIST_SPAN), 1)
    p_row = lax.broadcasted_iota(i32, (PAIRS_MAX, LIST_SPAN), 0)
    pieces = piece_ref[0:24, :].astype(bf16)
    for part in range(2):
        begin = column[0:ROWS, part:part + 1]
        end = begin + column[ROWS:2 * ROWS, part:part + 1]
        past = spot >= end
        inside = jnp.where((spot >= begin) & jnp.logical_not(past), f32(1), f32(0)).astype(bf16)
        past = jnp.where(past, f32(1), f32(0)).astype(bf16)
        chosen = lax.dot_general(pieces, inside, nn, preferred_element_type=f32)
        ahead = lax.dot_general(pairs, past, nn, preferred_element_type=f32)
        ahead = ahead[part:part + 1, :].astype(i32)
        pair = spot_row - ahead + 1
        mine = p_row == pair

        def field(at):
            return jnp.sum(
                jnp.where(mine, chosen[at:at + PAIRS_MAX, :], f32(0)), axis=0, keepdims=True
            ).astype(i32)

        item = (chosen[16:17, :].astype(i32) << 3) | (field(0) << 9) | (field(8) << 17)
        total = ahead[:, LIST_SPAN - 1:LIST_SPAN]
        item = jnp.where(spot_row < total, item | pair, 0)
        for block in range(LIST_BLOCKS):
            at = part * LIST_BLOCKS + block
            table_ref[at:at + 1, :] = item[:, block * 128:(block + 1) * 128]
        at = LENGTH_ROW + part
        table_ref[at:at + 1, :] = ahead[:, LIST_SPAN - 128:LIST_SPAN]


def pick_kernel(
    send_hbm, feat_hbm, cols_hbm, count_hbm, out_ref, slab_ref, table_ref, cols_out, count_out,
    send_ref, feat_ref, cols_ref, count_ref, piece_ref, sem,
):
    copies = [
        pltpu.make_async_copy(src, dst, sem.at[i])
        for i, (src, dst) in enumerate([
            (feat_hbm, feat_ref), (cols_hbm, cols_ref), (count_hbm, count_ref), (send_hbm, send_ref),
            (cols_hbm, cols_out), (count_hbm, count_out),
        ])
    ]
    for copy in copies:
        copy.start()
    slab_ref[0] = jnp.zeros(slab_ref.shape[1:], slab_ref.dtype)
    copies[1].wait()
    copies[2].wait()
    build_list(cols_ref, count_ref, piece_ref, table_ref)
    copies[3].wait()
    copies[0].wait()
    slots, peers = send_ref.shape
    for peer in range(peers):
        for slot in range(slots):
            start = pl.multiple_of(send_ref[slot, peer] * EDGE, EDGE)
            out_ref[peer * slots + slot] = feat_ref[:, pl.ds(start, EDGE)]
    for r in range(ROWS):
        slab_ref[r + 1] = feat_ref[:, r * EDGE:(r + 1) * EDGE]
    copies[4].wait()
    copies[5].wait()


def multiply_kernel(
    cols_ref, count_ref, table_ref, tiles_ref, own_ref, arrived_ref, out_ref, slab_ref,
    list_ref, even_ref, odd_ref, sem,
):
    to_smem = pltpu.make_async_copy(table_ref, list_ref, sem)
    to_smem.start()
    slab_ref[ROWS + 1:] = arrived_ref[...]
    contract = (((1,), (1,)), ((), ()))

    def product(part, both, a, b):
        tile = jnp.concatenate([tiles_ref[2 * both], tiles_ref[2 * both + 1]], axis=1)
        slab = jnp.concatenate([slab_ref[a], slab_ref[b]], axis=1)
        left, right = (tile, slab) if part == 0 else (slab, tile)
        return lax.dot_general(left, right, contract, preferred_element_type=jnp.float32)

    sums = (even_ref, odd_ref)
    for first in range(0, ROWS, 4):
        for part in range(2):
            for row in (first + part, first + part + 2):
                a = cols_ref[0, row] + 1
                b = jnp.where(count_ref[0, row] > 1, cols_ref[1, row] + 1, 0)
                sums[part][row // 2] = product(part, row * PAIRS_MAX, a, b)
    to_smem.wait()

    def chunk(i, carry):
        for u in range(0, EACH, 2):
            for part in range(2):
                for v in range(2):
                    at = i * EACH + u + v
                    item = list_ref[part * LIST_BLOCKS + (at >> 7), at & 127]
                    sums[part][(item >> 4) & 31] += product(
                        part, item & 511, (item >> 9) & 255, item >> 17
                    )
        return carry

    longest = jnp.maximum(list_ref[LENGTH_ROW, 127], list_ref[LENGTH_ROW + 1, 127])
    lax.fori_loop(0, (longest + (EACH - 1)) // EACH, chunk, 0)
    owners = out_ref.shape[0]
    each = ROWS // owners
    for row in range(HALF):
        owner, j = divmod(2 * row, each)
        out_ref[owner, :, j * EDGE:(j + 1) * EDGE] = even_ref[row].astype(out_ref.dtype).T
        out_ref[owner, :, (j + 1) * EDGE:(j + 2) * EDGE] = odd_ref[row].astype(out_ref.dtype)


def per_device(features, tiles, tile_cols, tile_count, send_list, weight, bias):
    block_count, tile_depth, edge, _ = tiles.shape
    width = features.shape[1]
    feat_count = lax.axis_size("feat")
    vert_count = lax.axis_size("vert")
    bf16, f32, i32 = jnp.bfloat16, jnp.float32, jnp.int32
    whole = pl.BlockSpec(memory_space=VMEM)
    scalar = pl.BlockSpec(memory_space=SMEM)
    in_hbm = pl.BlockSpec(memory_space=pltpu.HBM)
    dma = pltpu.SemaphoreType.DMA
    mib = 1024 * 1024

    def stay(x):
        return pltpu.with_memory_space_constraint(x, pltpu.HBM)

    flat_tiles = pltpu.with_memory_space_constraint(
        tiles.reshape(block_count * tile_depth, edge, edge), VMEM
    )

    chosen, slabs, table, cols, counts = pl.pallas_call(
        pick_kernel,
        out_shape=(
            VMEM((block_count, width, edge), bf16),
            VMEM((SLOTS, width, edge), bf16),
            VMEM((LIST_ROWS, 128), i32),
            SMEM((tile_depth, block_count), i32),
            SMEM((1, block_count), i32),
        ),
        in_specs=[in_hbm] * 4,
        out_specs=(whole, whole, whole, scalar, scalar),
        scratch_shapes=[
            SMEM(send_list.shape[:0:-1], i32),
            VMEM((width, block_count * edge), bf16),
            VMEM((tile_depth, block_count), i32),
            VMEM((1, block_count), i32),
            VMEM((32, block_count), f32),
            dma((6,)),
        ],
        name="pick",
        compiler_params=pltpu.CompilerParams(vmem_limit_bytes=4 * mib),
        cost_estimate=pl.CostEstimate(flops=20_000_000_000, bytes_accessed=200_000_000, transcendentals=0),
    )(
        stay(send_list[0].T), stay(features.T), stay(tile_cols.T),
        stay(tile_count.reshape(1, block_count)),
    )
    arrived = lax.all_to_all(
        chosen.reshape(vert_count, -1, width, edge), "vert", split_axis=0, concat_axis=0, tiled=True
    ).reshape(block_count, width, edge)

    hidden, _ = pl.pallas_call(
        multiply_kernel,
        out_shape=(
            jax.ShapeDtypeStruct((feat_count, width, block_count * edge // feat_count), bf16),
            VMEM((SLOTS, width, edge), bf16),
        ),
        in_specs=[scalar, scalar, whole, whole, whole, whole],
        out_specs=(whole, whole),
        scratch_shapes=[
            SMEM((LIST_ROWS, 128), i32),
            VMEM((HALF, edge, width), f32),
            VMEM((HALF, width, edge), f32),
            dma,
        ],
        input_output_aliases={4: 1},
        name="multiply",
        compiler_params=pltpu.CompilerParams(
            vmem_limit_bytes=8 * mib,
        ),
        cost_estimate=pl.CostEstimate(
            flops=8_000_000_000, bytes_accessed=17_000_000, transcendentals=0
        ),
    )(cols, counts, table, flat_tiles, slabs, arrived)

    full_rows = lax.all_to_all(hidden, "feat", split_axis=0, concat_axis=0, tiled=True)
    full_rows = full_rows.reshape(feat_count * width, -1)
    mixed_rows = lax.dot_general(
        full_rows, weight, (((0,), (0,)), ((), ())), preferred_element_type=f32
    )
    return jnp.maximum(mixed_rows + bias, f32(0.0)).astype(bf16)


def solution(mesh):
    return jax.shard_map(
        per_device,
        mesh=mesh,
        in_specs=(
            P("vert", "feat"),
            P("vert", None, None, None),
            P("vert", None),
            P("vert"),
            P("vert", None, None),
            P(),
            P(),
        ),
        out_specs=P(("vert", "feat"), None),
        check_vma=False,
    )
```

```python
import jax
import jax.numpy as jnp
from jax import lax
from jax.experimental import pallas as pl
from jax.experimental.pallas import tpu as pltpu
from jax.sharding import PartitionSpec as P

VMEM = pltpu.VMEM
SMEM = pltpu.SMEM
EACH = 32
VERT_LEAD = 10
FEAT_LEAD = 8
PAIRS_MAX = 8
ROWS = 64
HALF = ROWS // 2
EDGE = 128
SLOTS = 2 * ROWS + 1
SLOTS_EACH = 4
LIST_ROWS = 8
LIST_BLOCKS = 2
LIST_SPAN = LIST_BLOCKS * 128
LENGTH_ROW = 2 * LIST_BLOCKS


def led_by(lead, count):
    return [(lead + i) % count for i in range(count)]


def build_list(cols_ref, count_ref, piece_ref, table_ref):
    f32, i32, bf16 = jnp.float32, jnp.int32, jnp.bfloat16
    counts = count_ref[...]
    lane_row = lax.broadcasted_iota(i32, (1, ROWS), 1)
    for p in range(PAIRS_MAX):
        for half in range(2):
            k = 2 * p + half
            slot = jnp.where(counts > k, cols_ref[k:k + 1, :] + 1, 0)
            piece_ref[8 * half + p:8 * half + p + 1, :] = slot.astype(f32)
    piece_ref[16:17, :] = lane_row.astype(f32)
    piece_ref[17:24, :] = jnp.zeros((7, ROWS), f32)
    pairs_each = ((counts - 1) >> 1).astype(f32)
    odd = lane_row & 1
    for part in range(2):
        piece_ref[24 + part:25 + part, :] = jnp.where(odd == part, pairs_each, f32(0))
    piece_ref[26:32, :] = jnp.zeros((6, ROWS), f32)

    pairs = piece_ref[24:32, :].astype(bf16)
    r_out = lax.broadcasted_iota(i32, (2 * ROWS, ROWS), 0)
    r_in = lax.broadcasted_iota(i32, (2 * ROWS, ROWS), 1)
    before = jnp.where(r_out < ROWS, (r_in < r_out).astype(f32), (r_in == r_out - ROWS).astype(f32))
    nt = (((1,), (1,)), ((), ()))
    nn = (((1,), (0,)), ((), ()))
    column = lax.dot_general(before.astype(bf16), pairs, nt, preferred_element_type=f32)
    spot = lax.broadcasted_iota(i32, (ROWS, LIST_SPAN), 1).astype(f32)
    spot_row = lax.broadcasted_iota(i32, (1, LIST_SPAN), 1)
    p_row = lax.broadcasted_iota(i32, (PAIRS_MAX, LIST_SPAN), 0)
    pieces = piece_ref[0:24, :].astype(bf16)
    for part in range(2):
        begin = column[0:ROWS, part:part + 1]
        end = begin + column[ROWS:2 * ROWS, part:part + 1]
        past = spot >= end
        inside = jnp.where((spot >= begin) & jnp.logical_not(past), f32(1), f32(0)).astype(bf16)
        past = jnp.where(past, f32(1), f32(0)).astype(bf16)
        chosen = lax.dot_general(pieces, inside, nn, preferred_element_type=f32)
        ahead = lax.dot_general(pairs, past, nn, preferred_element_type=f32)
        ahead = ahead[part:part + 1, :].astype(i32)
        pair = spot_row - ahead + 1
        mine = p_row == pair

        def field(at):
            return jnp.sum(
                jnp.where(mine, chosen[at:at + PAIRS_MAX, :], f32(0)), axis=0, keepdims=True
            ).astype(i32)

        item = (chosen[16:17, :].astype(i32) << 3) | (field(0) << 9) | (field(8) << 17)
        total = ahead[:, LIST_SPAN - 1:LIST_SPAN]
        item = jnp.where(spot_row < total, item | pair, 0)
        for block in range(LIST_BLOCKS):
            at = part * LIST_BLOCKS + block
            table_ref[at:at + 1, :] = item[:, block * 128:(block + 1) * 128]
        at = LENGTH_ROW + part
        table_ref[at:at + 1, :] = ahead[:, LIST_SPAN - 128:LIST_SPAN]


def pick_kernel(
    send_hbm, feat_hbm, cols_hbm, count_hbm, weight_hbm,
    out_ref, slab_ref, table_ref, cols_out, count_out, weight_ref,
    send_ref, feat_ref, cols_ref, count_ref, piece_ref, sem,
):
    cut = FEAT_LEAD * out_ref.shape[1]
    rest = weight_ref.shape[0] - cut
    copies = [
        pltpu.make_async_copy(src, dst, sem.at[i])
        for i, (src, dst) in enumerate([
            (feat_hbm, feat_ref), (cols_hbm, cols_ref), (count_hbm, count_ref), (send_hbm, send_ref),
            (cols_hbm, cols_out), (count_hbm, count_out),
            (weight_hbm.at[pl.ds(cut, rest)], weight_ref.at[pl.ds(0, rest)]),
            (weight_hbm.at[pl.ds(0, cut)], weight_ref.at[pl.ds(rest, cut)]),
        ])
    ]
    for copy in copies:
        copy.start()
    slab_ref[0] = jnp.zeros(slab_ref.shape[1:], slab_ref.dtype)
    copies[1].wait()
    copies[2].wait()
    build_list(cols_ref, count_ref, piece_ref, table_ref)
    copies[3].wait()
    copies[0].wait()
    slots, peers = send_ref.shape
    for at, peer in enumerate(led_by(VERT_LEAD, peers)):
        for slot in range(slots):
            start = pl.multiple_of(send_ref[slot, peer] * EDGE, EDGE)
            out_ref[at * slots + slot] = feat_ref[:, pl.ds(start, EDGE)]
    for r in range(ROWS):
        slab_ref[r + 1] = feat_ref[:, r * EDGE:(r + 1) * EDGE]
    for copy in copies[4:]:
        copy.wait()


def multiply_kernel(
    cols_ref, count_ref, table_ref, tiles_ref, own_ref, arrived_ref, out_ref, slab_ref,
    list_ref, even_ref, odd_ref, sem,
):
    to_smem = pltpu.make_async_copy(table_ref, list_ref, sem)
    to_smem.start()
    cut = VERT_LEAD * SLOTS_EACH
    slab_ref[ROWS + 1:ROWS + 1 + cut] = arrived_ref[ROWS - cut:]
    slab_ref[ROWS + 1 + cut:] = arrived_ref[:ROWS - cut]
    contract = (((1,), (1,)), ((), ()))

    def product(part, both, a, b):
        tile = jnp.concatenate([tiles_ref[2 * both], tiles_ref[2 * both + 1]], axis=1)
        slab = jnp.concatenate([slab_ref[a], slab_ref[b]], axis=1)
        left, right = (tile, slab) if part == 0 else (slab, tile)
        return lax.dot_general(left, right, contract, preferred_element_type=jnp.float32)

    sums = (even_ref, odd_ref)
    for first in range(0, ROWS, 4):
        for part in range(2):
            for row in (first + part, first + part + 2):
                a = cols_ref[0, row] + 1
                b = jnp.where(count_ref[0, row] > 1, cols_ref[1, row] + 1, 0)
                sums[part][row // 2] = product(part, row * PAIRS_MAX, a, b)
    to_smem.wait()

    def chunk(i, carry):
        for u in range(0, EACH, 2):
            for part in range(2):
                for v in range(2):
                    at = i * EACH + u + v
                    item = list_ref[part * LIST_BLOCKS + (at >> 7), at & 127]
                    sums[part][(item >> 4) & 31] += product(
                        part, item & 511, (item >> 9) & 255, item >> 17
                    )
        return carry

    longest = jnp.maximum(list_ref[LENGTH_ROW, 127], list_ref[LENGTH_ROW + 1, 127])
    lax.fori_loop(0, (longest + (EACH - 1)) // EACH, chunk, 0)
    owners = out_ref.shape[0]
    each = ROWS // owners
    place = {owner: at for at, owner in enumerate(led_by(FEAT_LEAD, owners))}
    for row in range(HALF):
        owner, j = divmod(2 * row, each)
        owner = place[owner]
        out_ref[owner, :, j * EDGE:(j + 1) * EDGE] = even_ref[row].astype(out_ref.dtype).T
        out_ref[owner, :, (j + 1) * EDGE:(j + 2) * EDGE] = odd_ref[row].astype(out_ref.dtype)


def per_device(features, tiles, tile_cols, tile_count, send_list, weight, bias):
    block_count, tile_depth, edge, _ = tiles.shape
    width = features.shape[1]
    feat_count = lax.axis_size("feat")
    vert_count = lax.axis_size("vert")
    bf16, f32, i32 = jnp.bfloat16, jnp.float32, jnp.int32
    whole = pl.BlockSpec(memory_space=VMEM)
    scalar = pl.BlockSpec(memory_space=SMEM)
    in_hbm = pl.BlockSpec(memory_space=pltpu.HBM)
    dma = pltpu.SemaphoreType.DMA
    mib = 1024 * 1024

    def stay(x):
        return pltpu.with_memory_space_constraint(x, pltpu.HBM)

    flat_tiles = pltpu.with_memory_space_constraint(
        tiles.reshape(block_count * tile_depth, edge, edge), VMEM
    )

    chosen, slabs, table, cols, counts, turned_weight = pl.pallas_call(
        pick_kernel,
        out_shape=(
            VMEM((block_count, width, edge), bf16),
            VMEM((SLOTS, width, edge), bf16),
            VMEM((LIST_ROWS, 128), i32),
            SMEM((tile_depth, block_count), i32),
            SMEM((1, block_count), i32),
            VMEM(weight.shape, bf16),
        ),
        in_specs=[in_hbm] * 5,
        out_specs=(whole, whole, whole, scalar, scalar, whole),
        scratch_shapes=[
            SMEM(send_list.shape[:0:-1], i32),
            VMEM((width, block_count * edge), bf16),
            VMEM((tile_depth, block_count), i32),
            VMEM((1, block_count), i32),
            VMEM((32, block_count), f32),
            dma((8,)),
        ],
        name="pick",
        compiler_params=pltpu.CompilerParams(vmem_limit_bytes=4 * mib),
        cost_estimate=pl.CostEstimate(flops=20_000_000_000, bytes_accessed=200_000_000, transcendentals=0),
    )(
        stay(send_list[0].T), stay(features.T), stay(tile_cols.T),
        stay(tile_count.reshape(1, block_count)), stay(weight),
    )
    arrived = lax.all_to_all(
        chosen.reshape(vert_count, -1, width, edge), "vert", split_axis=0, concat_axis=0, tiled=True,
        axis_index_groups=[led_by(VERT_LEAD, vert_count)],
    ).reshape(block_count, width, edge)

    hidden, _ = pl.pallas_call(
        multiply_kernel,
        out_shape=(
            jax.ShapeDtypeStruct((feat_count, width, block_count * edge // feat_count), bf16),
            VMEM((SLOTS, width, edge), bf16),
        ),
        in_specs=[scalar, scalar, whole, whole, whole, whole],
        out_specs=(whole, whole),
        scratch_shapes=[
            SMEM((LIST_ROWS, 128), i32),
            VMEM((HALF, edge, width), f32),
            VMEM((HALF, width, edge), f32),
            dma,
        ],
        input_output_aliases={4: 1},
        name="multiply",
        compiler_params=pltpu.CompilerParams(
            vmem_limit_bytes=8 * mib,
        ),
        cost_estimate=pl.CostEstimate(
            flops=8_000_000_000, bytes_accessed=17_000_000, transcendentals=0
        ),
    )(cols, counts, table, flat_tiles, slabs, arrived)

    full_rows = lax.all_to_all(
        hidden, "feat", split_axis=0, concat_axis=0, tiled=True,
        axis_index_groups=[led_by(FEAT_LEAD, feat_count)],
    )
    full_rows = full_rows.reshape(feat_count * width, -1)
    mixed_rows = lax.dot_general(
        full_rows, turned_weight, (((0,), (0,)), ((), ())), preferred_element_type=f32
    )
    return jnp.maximum(mixed_rows + bias, f32(0.0)).astype(bf16)


def solution(mesh):
    return jax.shard_map(
        per_device,
        mesh=mesh,
        in_specs=(
            P("vert", "feat"),
            P("vert", None, None, None),
            P("vert", None),
            P("vert"),
            P("vert", None, None),
            P(),
            P(),
        ),
        out_specs=P(("vert", "feat"), None),
        check_vma=False,
    )
```

```python
import jax
import jax.numpy as jnp
from jax import lax
from jax.experimental import pallas as pl
from jax.experimental.pallas import tpu as pltpu
from jax.sharding import PartitionSpec as P

VMEM = pltpu.VMEM
SMEM = pltpu.SMEM
EACH = 32
VERT_LEAD = 10
FEAT_LEAD = 8
PAIRS_MAX = 8
ROWS = 64
HALF = ROWS // 2
EDGE = 128
SLOTS = 2 * ROWS + 1
SLOTS_EACH = 4
LIST_ROWS = 8
LIST_BLOCKS = 2
LIST_SPAN = LIST_BLOCKS * 128
LENGTH_ROW = 2 * LIST_BLOCKS


def led_by(lead, count):
    return [(lead + i) % count for i in range(count)]


def build_list(cols_ref, count_ref, piece_ref, table_ref):
    f32, i32, bf16 = jnp.float32, jnp.int32, jnp.bfloat16
    counts = count_ref[...]
    lane_row = lax.broadcasted_iota(i32, (1, ROWS), 1)
    for p in range(PAIRS_MAX):
        for half in range(2):
            k = 2 * p + half
            slot = jnp.where(counts > k, cols_ref[k:k + 1, :] + 1, 0)
            piece_ref[8 * half + p:8 * half + p + 1, :] = slot.astype(f32)
    piece_ref[16:17, :] = lane_row.astype(f32)
    piece_ref[17:24, :] = jnp.zeros((7, ROWS), f32)
    pairs_each = ((counts - 1) >> 1).astype(f32)
    odd = lane_row & 1
    for part in range(2):
        piece_ref[24 + part:25 + part, :] = jnp.where(odd == part, pairs_each, f32(0))
    piece_ref[26:32, :] = jnp.zeros((6, ROWS), f32)

    pairs = piece_ref[24:32, :].astype(bf16)
    r_out = lax.broadcasted_iota(i32, (2 * ROWS, ROWS), 0)
    r_in = lax.broadcasted_iota(i32, (2 * ROWS, ROWS), 1)
    before = jnp.where(r_out < ROWS, (r_in < r_out).astype(f32), (r_in == r_out - ROWS).astype(f32))
    nt = (((1,), (1,)), ((), ()))
    nn = (((1,), (0,)), ((), ()))
    column = lax.dot_general(before.astype(bf16), pairs, nt, preferred_element_type=f32)
    spot = lax.broadcasted_iota(i32, (ROWS, LIST_SPAN), 1).astype(f32)
    spot_row = lax.broadcasted_iota(i32, (1, LIST_SPAN), 1)
    p_row = lax.broadcasted_iota(i32, (PAIRS_MAX, LIST_SPAN), 0)
    pieces = piece_ref[0:24, :].astype(bf16)
    for part in range(2):
        begin = column[0:ROWS, part:part + 1]
        end = begin + column[ROWS:2 * ROWS, part:part + 1]
        past = spot >= end
        inside = jnp.where((spot >= begin) & jnp.logical_not(past), f32(1), f32(0)).astype(bf16)
        past = jnp.where(past, f32(1), f32(0)).astype(bf16)
        chosen = lax.dot_general(pieces, inside, nn, preferred_element_type=f32)
        ahead = lax.dot_general(pairs, past, nn, preferred_element_type=f32)
        ahead = ahead[part:part + 1, :].astype(i32)
        pair = spot_row - ahead + 1
        mine = p_row == pair

        def field(at):
            return jnp.sum(
                jnp.where(mine, chosen[at:at + PAIRS_MAX, :], f32(0)), axis=0, keepdims=True
            ).astype(i32)

        item = (chosen[16:17, :].astype(i32) << 3) | (field(0) << 9) | (field(8) << 17)
        total = ahead[:, LIST_SPAN - 1:LIST_SPAN]
        item = jnp.where(spot_row < total, item | pair, 0)
        for block in range(LIST_BLOCKS):
            at = part * LIST_BLOCKS + block
            table_ref[at:at + 1, :] = item[:, block * 128:(block + 1) * 128]
        at = LENGTH_ROW + part
        table_ref[at:at + 1, :] = ahead[:, LIST_SPAN - 128:LIST_SPAN]


def pick_kernel(
    send_hbm, feat_hbm, cols_hbm, count_hbm, weight_hbm,
    out_ref, slab_ref, table_ref, cols_out, count_out, weight_ref,
    send_ref, feat_ref, cols_ref, count_ref, piece_ref, sem,
):
    cut = FEAT_LEAD * out_ref.shape[1]
    rest = weight_ref.shape[0] - cut
    copies = [
        pltpu.make_async_copy(src, dst, sem.at[i])
        for i, (src, dst) in enumerate([
            (feat_hbm, feat_ref), (cols_hbm, cols_ref), (count_hbm, count_ref), (send_hbm, send_ref),
            (cols_hbm, cols_out), (count_hbm, count_out),
            (weight_hbm.at[pl.ds(cut, rest)], weight_ref.at[pl.ds(0, rest)]),
            (weight_hbm.at[pl.ds(0, cut)], weight_ref.at[pl.ds(rest, cut)]),
        ])
    ]
    for i in (3, 1, 2, 0, 4, 5, 6, 7):
        copies[i].start()
    slab_ref[0] = jnp.zeros(slab_ref.shape[1:], slab_ref.dtype)
    copies[1].wait()
    copies[2].wait()
    build_list(cols_ref, count_ref, piece_ref, table_ref)
    copies[3].wait()
    copies[0].wait()
    slots, peers = send_ref.shape
    for at, peer in enumerate(led_by(VERT_LEAD, peers)):
        for slot in range(slots):
            start = pl.multiple_of(send_ref[slot, peer] * EDGE, EDGE)
            out_ref[at * slots + slot] = feat_ref[:, pl.ds(start, EDGE)]
    for r in range(ROWS):
        slab_ref[r + 1] = feat_ref[:, r * EDGE:(r + 1) * EDGE]
    for copy in copies[4:]:
        copy.wait()


def multiply_kernel(
    cols_ref, count_ref, table_ref, tiles_ref, own_ref, arrived_ref, out_ref, slab_ref,
    list_ref, even_ref, odd_ref, sem,
):
    to_smem = pltpu.make_async_copy(table_ref, list_ref, sem)
    to_smem.start()
    cut = VERT_LEAD * SLOTS_EACH
    slab_ref[ROWS + 1:ROWS + 1 + cut] = arrived_ref[ROWS - cut:]
    slab_ref[ROWS + 1 + cut:] = arrived_ref[:ROWS - cut]
    contract = (((1,), (1,)), ((), ()))

    def product(part, both, a, b):
        tile = jnp.concatenate([tiles_ref[2 * both], tiles_ref[2 * both + 1]], axis=1)
        slab = jnp.concatenate([slab_ref[a], slab_ref[b]], axis=1)
        left, right = (tile, slab) if part == 0 else (slab, tile)
        return lax.dot_general(left, right, contract, preferred_element_type=jnp.float32)

    sums = (even_ref, odd_ref)
    for first in range(0, ROWS, 4):
        for part in range(2):
            for row in (first + part, first + part + 2):
                a = cols_ref[0, row] + 1
                b = jnp.where(count_ref[0, row] > 1, cols_ref[1, row] + 1, 0)
                sums[part][row // 2] = product(part, row * PAIRS_MAX, a, b)
    to_smem.wait()

    def chunk(i, carry):
        for u in range(0, EACH, 2):
            for part in range(2):
                for v in range(2):
                    at = i * EACH + u + v
                    item = list_ref[part * LIST_BLOCKS + (at >> 7), at & 127]
                    sums[part][(item >> 4) & 31] += product(
                        part, item & 511, (item >> 9) & 255, item >> 17
                    )
        return carry

    longest = jnp.maximum(list_ref[LENGTH_ROW, 127], list_ref[LENGTH_ROW + 1, 127])
    lax.fori_loop(0, (longest + (EACH - 1)) // EACH, chunk, 0)
    owners = out_ref.shape[0]
    each = ROWS // owners
    place = {owner: at for at, owner in enumerate(led_by(FEAT_LEAD, owners))}
    for row in range(HALF):
        owner, j = divmod(2 * row, each)
        owner = place[owner]
        out_ref[owner, :, j * EDGE:(j + 1) * EDGE] = even_ref[row].astype(out_ref.dtype).T
        out_ref[owner, :, (j + 1) * EDGE:(j + 2) * EDGE] = odd_ref[row].astype(out_ref.dtype)


def per_device(features, tiles, tile_cols, tile_count, send_list, weight, bias):
    block_count, tile_depth, edge, _ = tiles.shape
    width = features.shape[1]
    feat_count = lax.axis_size("feat")
    vert_count = lax.axis_size("vert")
    bf16, f32, i32 = jnp.bfloat16, jnp.float32, jnp.int32
    whole = pl.BlockSpec(memory_space=VMEM)
    scalar = pl.BlockSpec(memory_space=SMEM)
    in_hbm = pl.BlockSpec(memory_space=pltpu.HBM)
    dma = pltpu.SemaphoreType.DMA
    mib = 1024 * 1024

    def stay(x):
        return pltpu.with_memory_space_constraint(x, pltpu.HBM)

    flat_tiles = pltpu.with_memory_space_constraint(
        tiles.reshape(block_count * tile_depth, edge, edge), VMEM
    )

    chosen, slabs, table, cols, counts, turned_weight = pl.pallas_call(
        pick_kernel,
        out_shape=(
            VMEM((block_count, width, edge), bf16),
            VMEM((SLOTS, width, edge), bf16),
            VMEM((LIST_ROWS, 128), i32),
            SMEM((tile_depth, block_count), i32),
            SMEM((1, block_count), i32),
            VMEM(weight.shape, bf16),
        ),
        in_specs=[in_hbm] * 5,
        out_specs=(whole, whole, whole, scalar, scalar, whole),
        scratch_shapes=[
            SMEM(send_list.shape[:0:-1], i32),
            VMEM((width, block_count * edge), bf16),
            VMEM((tile_depth, block_count), i32),
            VMEM((1, block_count), i32),
            VMEM((32, block_count), f32),
            dma((8,)),
        ],
        name="pick",
        compiler_params=pltpu.CompilerParams(vmem_limit_bytes=4 * mib),
        cost_estimate=pl.CostEstimate(flops=20_000_000_000, bytes_accessed=200_000_000, transcendentals=0),
    )(
        stay(send_list[0].T), stay(features.T), stay(tile_cols.T),
        stay(tile_count.reshape(1, block_count)), stay(weight),
    )
    arrived = lax.all_to_all(
        chosen.reshape(vert_count, -1, width, edge), "vert", split_axis=0, concat_axis=0, tiled=True,
        axis_index_groups=[led_by(VERT_LEAD, vert_count)],
    ).reshape(block_count, width, edge)

    hidden, _ = pl.pallas_call(
        multiply_kernel,
        out_shape=(
            jax.ShapeDtypeStruct((feat_count, width, block_count * edge // feat_count), bf16),
            VMEM((SLOTS, width, edge), bf16),
        ),
        in_specs=[scalar, scalar, whole, whole, whole, whole],
        out_specs=(whole, whole),
        scratch_shapes=[
            SMEM((LIST_ROWS, 128), i32),
            VMEM((HALF, edge, width), f32),
            VMEM((HALF, width, edge), f32),
            dma,
        ],
        input_output_aliases={4: 1},
        name="multiply",
        compiler_params=pltpu.CompilerParams(
            vmem_limit_bytes=8 * mib,
        ),
        cost_estimate=pl.CostEstimate(
            flops=8_000_000_000, bytes_accessed=17_000_000, transcendentals=0
        ),
    )(cols, counts, table, flat_tiles, slabs, arrived)

    full_rows = lax.all_to_all(
        hidden, "feat", split_axis=0, concat_axis=0, tiled=True,
        axis_index_groups=[led_by(FEAT_LEAD, feat_count)],
    )
    full_rows = full_rows.reshape(feat_count * width, -1)
    mixed_rows = lax.dot_general(
        full_rows, turned_weight, (((0,), (0,)), ((), ())), preferred_element_type=f32
    )
    return jnp.maximum(mixed_rows + bias, f32(0.0)).astype(bf16)


def solution(mesh):
    return jax.shard_map(
        per_device,
        mesh=mesh,
        in_specs=(
            P("vert", "feat"),
            P("vert", None, None, None),
            P("vert", None),
            P("vert"),
            P("vert", None, None),
            P(),
            P(),
        ),
        out_specs=P(("vert", "feat"), None),
        check_vma=False,
    )
```

```python
import jax
import jax.numpy as jnp
from jax import lax
from jax.experimental import pallas as pl
from jax.experimental.pallas import tpu as pltpu
from jax.sharding import PartitionSpec as P

VMEM = pltpu.VMEM
SMEM = pltpu.SMEM
EACH = 32
VERT_LEAD = 10
FEAT_LEAD = 9
PAIRS_MAX = 8
ROWS = 64
HALF = ROWS // 2
EDGE = 128
SLOTS = 2 * ROWS + 1
SLOTS_EACH = 4
LIST_ROWS = 8
LIST_BLOCKS = 2
LIST_SPAN = LIST_BLOCKS * 128
LENGTH_ROW = 2 * LIST_BLOCKS


def led_by(lead, count):
    return [(lead + i) % count for i in range(count)]


def build_list(cols_ref, count_ref, piece_ref, table_ref):
    f32, i32, bf16 = jnp.float32, jnp.int32, jnp.bfloat16
    counts = count_ref[...]
    lane_row = lax.broadcasted_iota(i32, (1, ROWS), 1)
    for p in range(PAIRS_MAX):
        for half in range(2):
            k = 2 * p + half
            slot = jnp.where(counts > k, cols_ref[k:k + 1, :] + 1, 0)
            piece_ref[8 * half + p:8 * half + p + 1, :] = slot.astype(f32)
    piece_ref[16:17, :] = lane_row.astype(f32)
    piece_ref[17:24, :] = jnp.zeros((7, ROWS), f32)
    pairs_each = ((counts - 1) >> 1).astype(f32)
    odd = lane_row & 1
    for part in range(2):
        piece_ref[24 + part:25 + part, :] = jnp.where(odd == part, pairs_each, f32(0))
    piece_ref[26:32, :] = jnp.zeros((6, ROWS), f32)

    pairs = piece_ref[24:32, :].astype(bf16)
    r_out = lax.broadcasted_iota(i32, (2 * ROWS, ROWS), 0)
    r_in = lax.broadcasted_iota(i32, (2 * ROWS, ROWS), 1)
    before = jnp.where(r_out < ROWS, (r_in < r_out).astype(f32), (r_in == r_out - ROWS).astype(f32))
    nt = (((1,), (1,)), ((), ()))
    nn = (((1,), (0,)), ((), ()))
    column = lax.dot_general(before.astype(bf16), pairs, nt, preferred_element_type=f32)
    spot = lax.broadcasted_iota(i32, (ROWS, LIST_SPAN), 1).astype(f32)
    spot_row = lax.broadcasted_iota(i32, (1, LIST_SPAN), 1)
    p_row = lax.broadcasted_iota(i32, (PAIRS_MAX, LIST_SPAN), 0)
    pieces = piece_ref[0:24, :].astype(bf16)
    for part in range(2):
        begin = column[0:ROWS, part:part + 1]
        end = begin + column[ROWS:2 * ROWS, part:part + 1]
        past = spot >= end
        inside = jnp.where((spot >= begin) & jnp.logical_not(past), f32(1), f32(0)).astype(bf16)
        past = jnp.where(past, f32(1), f32(0)).astype(bf16)
        chosen = lax.dot_general(pieces, inside, nn, preferred_element_type=f32)
        ahead = lax.dot_general(pairs, past, nn, preferred_element_type=f32)
        ahead = ahead[part:part + 1, :].astype(i32)
        pair = spot_row - ahead + 1
        mine = p_row == pair

        def field(at):
            return jnp.sum(
                jnp.where(mine, chosen[at:at + PAIRS_MAX, :], f32(0)), axis=0, keepdims=True
            ).astype(i32)

        item = (chosen[16:17, :].astype(i32) << 3) | (field(0) << 9) | (field(8) << 17)
        total = ahead[:, LIST_SPAN - 1:LIST_SPAN]
        item = jnp.where(spot_row < total, item | pair, 0)
        for block in range(LIST_BLOCKS):
            at = part * LIST_BLOCKS + block
            table_ref[at:at + 1, :] = item[:, block * 128:(block + 1) * 128]
        at = LENGTH_ROW + part
        table_ref[at:at + 1, :] = ahead[:, LIST_SPAN - 128:LIST_SPAN]


def pick_kernel(
    send_hbm, feat_hbm, cols_hbm, count_hbm, weight_hbm,
    out_ref, slab_ref, table_ref, cols_out, count_out, weight_ref,
    send_ref, feat_ref, cols_ref, count_ref, piece_ref, sem,
):
    cut = FEAT_LEAD * out_ref.shape[1]
    rest = weight_ref.shape[0] - cut
    copies = [
        pltpu.make_async_copy(src, dst, sem.at[i])
        for i, (src, dst) in enumerate([
            (feat_hbm, feat_ref), (cols_hbm, cols_ref), (count_hbm, count_ref), (send_hbm, send_ref),
            (cols_hbm, cols_out), (count_hbm, count_out),
            (weight_hbm.at[pl.ds(cut, rest)], weight_ref.at[pl.ds(0, rest)]),
            (weight_hbm.at[pl.ds(0, cut)], weight_ref.at[pl.ds(rest, cut)]),
        ])
    ]
    for copy in copies:
        copy.start()
    slab_ref[0] = jnp.zeros(slab_ref.shape[1:], slab_ref.dtype)
    copies[1].wait()
    copies[2].wait()
    build_list(cols_ref, count_ref, piece_ref, table_ref)
    copies[3].wait()
    copies[0].wait()
    slots, peers = send_ref.shape
    for at, peer in enumerate(led_by(VERT_LEAD, peers)):
        for slot in range(slots):
            start = pl.multiple_of(send_ref[slot, peer] * EDGE, EDGE)
            out_ref[at * slots + slot] = feat_ref[:, pl.ds(start, EDGE)]
    for r in range(ROWS):
        slab_ref[r + 1] = feat_ref[:, r * EDGE:(r + 1) * EDGE]
    for copy in copies[4:]:
        copy.wait()


def multiply_kernel(
    cols_ref, count_ref, table_ref, tiles_ref, own_ref, arrived_ref, out_ref, slab_ref,
    list_ref, even_ref, odd_ref, sem,
):
    to_smem = pltpu.make_async_copy(table_ref, list_ref, sem)
    to_smem.start()
    cut = VERT_LEAD * SLOTS_EACH
    slab_ref[ROWS + 1:ROWS + 1 + cut] = arrived_ref[ROWS - cut:]
    slab_ref[ROWS + 1 + cut:] = arrived_ref[:ROWS - cut]
    contract = (((1,), (1,)), ((), ()))

    def product(part, both, a, b):
        tile = jnp.concatenate([tiles_ref[2 * both], tiles_ref[2 * both + 1]], axis=1)
        slab = jnp.concatenate([slab_ref[a], slab_ref[b]], axis=1)
        left, right = (tile, slab) if part == 0 else (slab, tile)
        return lax.dot_general(left, right, contract, preferred_element_type=jnp.float32)

    sums = (even_ref, odd_ref)
    for first in range(0, ROWS, 4):
        for part in range(2):
            for row in (first + part, first + part + 2):
                a = cols_ref[0, row] + 1
                b = jnp.where(count_ref[0, row] > 1, cols_ref[1, row] + 1, 0)
                sums[part][row // 2] = product(part, row * PAIRS_MAX, a, b)
    to_smem.wait()

    def chunk(i, carry):
        for u in range(0, EACH, 2):
            for part in range(2):
                for v in range(2):
                    at = i * EACH + u + v
                    item = list_ref[part * LIST_BLOCKS + (at >> 7), at & 127]
                    sums[part][(item >> 4) & 31] += product(
                        part, item & 511, (item >> 9) & 255, item >> 17
                    )
        return carry

    longest = jnp.maximum(list_ref[LENGTH_ROW, 127], list_ref[LENGTH_ROW + 1, 127])
    lax.fori_loop(0, (longest + (EACH - 1)) // EACH, chunk, 0)
    owners = out_ref.shape[0]
    each = ROWS // owners
    place = {owner: at for at, owner in enumerate(led_by(FEAT_LEAD, owners))}
    for row in range(HALF):
        owner, j = divmod(2 * row, each)
        owner = place[owner]
        out_ref[owner, :, j * EDGE:(j + 1) * EDGE] = even_ref[row].astype(out_ref.dtype).T
        out_ref[owner, :, (j + 1) * EDGE:(j + 2) * EDGE] = odd_ref[row].astype(out_ref.dtype)


def per_device(features, tiles, tile_cols, tile_count, send_list, weight, bias):
    block_count, tile_depth, edge, _ = tiles.shape
    width = features.shape[1]
    feat_count = lax.axis_size("feat")
    vert_count = lax.axis_size("vert")
    bf16, f32, i32 = jnp.bfloat16, jnp.float32, jnp.int32
    whole = pl.BlockSpec(memory_space=VMEM)
    scalar = pl.BlockSpec(memory_space=SMEM)
    in_hbm = pl.BlockSpec(memory_space=pltpu.HBM)
    dma = pltpu.SemaphoreType.DMA
    mib = 1024 * 1024

    def stay(x):
        return pltpu.with_memory_space_constraint(x, pltpu.HBM)

    flat_tiles = pltpu.with_memory_space_constraint(
        tiles.reshape(block_count * tile_depth, edge, edge), VMEM
    )

    chosen, slabs, table, cols, counts, turned_weight = pl.pallas_call(
        pick_kernel,
        out_shape=(
            VMEM((block_count, width, edge), bf16),
            VMEM((SLOTS, width, edge), bf16),
            VMEM((LIST_ROWS, 128), i32),
            SMEM((tile_depth, block_count), i32),
            SMEM((1, block_count), i32),
            VMEM(weight.shape, bf16),
        ),
        in_specs=[in_hbm] * 5,
        out_specs=(whole, whole, whole, scalar, scalar, whole),
        scratch_shapes=[
            SMEM(send_list.shape[:0:-1], i32),
            VMEM((width, block_count * edge), bf16),
            VMEM((tile_depth, block_count), i32),
            VMEM((1, block_count), i32),
            VMEM((32, block_count), f32),
            dma((8,)),
        ],
        name="pick",
        compiler_params=pltpu.CompilerParams(vmem_limit_bytes=4 * mib),
        cost_estimate=pl.CostEstimate(flops=20_000_000_000, bytes_accessed=200_000_000, transcendentals=0),
    )(
        stay(send_list[0].T), stay(features.T), stay(tile_cols.T),
        stay(tile_count.reshape(1, block_count)), stay(weight),
    )
    arrived = lax.all_to_all(
        chosen.reshape(vert_count, -1, width, edge), "vert", split_axis=0, concat_axis=0, tiled=True,
        axis_index_groups=[led_by(VERT_LEAD, vert_count)],
    ).reshape(block_count, width, edge)

    hidden, _ = pl.pallas_call(
        multiply_kernel,
        out_shape=(
            jax.ShapeDtypeStruct((feat_count, width, block_count * edge // feat_count), bf16),
            VMEM((SLOTS, width, edge), bf16),
        ),
        in_specs=[scalar, scalar, whole, whole, whole, whole],
        out_specs=(whole, whole),
        scratch_shapes=[
            SMEM((LIST_ROWS, 128), i32),
            VMEM((HALF, edge, width), f32),
            VMEM((HALF, width, edge), f32),
            dma,
        ],
        input_output_aliases={4: 1},
        name="multiply",
        compiler_params=pltpu.CompilerParams(
            vmem_limit_bytes=8 * mib,
        ),
        cost_estimate=pl.CostEstimate(
            flops=8_000_000_000, bytes_accessed=17_000_000, transcendentals=0
        ),
    )(cols, counts, table, flat_tiles, slabs, arrived)

    full_rows = lax.all_to_all(
        hidden, "feat", split_axis=0, concat_axis=0, tiled=True,
        axis_index_groups=[led_by(FEAT_LEAD, feat_count)],
    )
    full_rows = full_rows.reshape(feat_count * width, -1)
    mixed_rows = lax.dot_general(
        full_rows, turned_weight, (((0,), (0,)), ((), ())), preferred_element_type=f32
    )
    return jnp.maximum(mixed_rows + bias, f32(0.0)).astype(bf16)


def solution(mesh):
    return jax.shard_map(
        per_device,
        mesh=mesh,
        in_specs=(
            P("vert", "feat"),
            P("vert", None, None, None),
            P("vert", None),
            P("vert"),
            P("vert", None, None),
            P(),
            P(),
        ),
        out_specs=P(("vert", "feat"), None),
        check_vma=False,
    )
```
